512 devices in a mesh: mp: 8 (over x, z_hi), tok: 64 (over y, z_lo, core).
Axes of the slice: x: 4, y: 4, z: 16 (z_hi: 2, z_lo: 8; z = z_hi * 8 + z_lo), core: 2. Of those that a mesh axis runs over, the one named last changes fastest.
Arguments:
- inputs: bfloat16 [8, 64, 128, 2048], P('mp', 'tok'), may hold values from -6 to 6
- cotangent: bfloat16 [8, 64, 128, 4096], P('mp', 'tok'), may hold values from -6 to 6
- token_ids: int32 [8, 64, 128], P('mp', 'tok'), may hold values from 0 to 151935
- weights: float32 [8, 64, 256, 512], P('mp', 'tok'), may hold values from -6 to 6
Outputs:
- merged: float32 [64, 256, 512], P('tok')
The draws below stay inside these ranges and needn't reach their ends.
All inputs are finite; a program needn't handle non-finite values.
Results may differ from the reference program's by a relative error of at most 0.0003.
Values may be sent and summed in bfloat16 or wider, within the bound.
A program may use at most 64 MiB of HBM per device.

```python
import math
import jax
import jax.numpy as jnp
from jax import lax

D = 2048
Q = 4096
VOCAB = 151936
TOK_SEQ = 128
ROW_BLOCKS = 8
FIRST_TEXT = 37984
MODELS = 8
SEQS = 64
BLOCKS = 64
COL_BLOCKS = 8
ROW_SPAN = 256
COL_SPAN = 512


def touch_ends(values, own_key, least, largest):
    dims = values.shape
    spot = [jax.random.randint(jax.random.fold_in(own_key, axis), (), 0, dims[axis]) for axis in range(len(dims))]
    values = values.at[tuple(spot)].set(least)
    longest = dims.index(max(dims))
    spot[longest] = (spot[longest] + 1) % dims[longest]
    return values.at[tuple(spot)].set(largest)


def levels(key, shape, shards, least, high):
    level, own = 1.0, jax.random.fold_in(key, 6)
    for axis_at, shards_of in shards:
        heights = jnp.exp(jax.random.uniform(jax.random.fold_in(own, axis_at), (shards_of,), jnp.float32, least / len(shards), high / len(shards)))
        level = level * jnp.repeat(heights, shape[axis_at] // shards_of).reshape([-1 if axis == axis_at else 1 for axis in range(len(shape))])
    return level


def centred(own_key, shape, scale, bound, shards=(), held_as=jnp.bfloat16):
    result = scale * jax.random.normal(own_key, shape, jnp.float32)
    if shards:
        result = result * levels(own_key, shape, shards, -0.22, 0.18)
    return jnp.clip(result, -bound, bound).astype(held_as)


def setup_inputs(seed: int = 0) -> dict:
    keys = jax.random.split(jax.random.key(seed), 5)
    return {
        "inputs": centred(keys[0], (MODELS, SEQS, TOK_SEQ, D), 1.0, 6.0, ((0, 8), (1, 64))),
        "cotangent": centred(keys[1], (MODELS, SEQS, TOK_SEQ, Q), 1.0, 6.0, ((0, 8), (1, 64))),
        "token_ids": touch_ends(jax.random.randint(keys[2], (MODELS, SEQS, TOK_SEQ), 0, VOCAB), jax.random.fold_in(keys[2], 1), 0, VOCAB - 1).astype(jnp.int32),
        "weights": centred(keys[3], (MODELS, BLOCKS, ROW_SPAN, COL_SPAN), 1.0, 6.0, ((0, 8), (1, 64)), jnp.float32),
    }


damping = 0.1

def one_model(bundle):
    activations, cotangents, identifiers = bundle

    def accumulate(summed, sequence):
        act_rows, cot_rows, id_rows = sequence
        kept_mask = (id_rows >= FIRST_TEXT).astype(jnp.bfloat16)
        masked = cot_rows * kept_mask[:, None]
        gradient = jnp.dot(act_rows.T, masked, preferred_element_type=jnp.float32) / math.sqrt(TOK_SEQ)
        return (summed + gradient * gradient, None)
    start = jnp.zeros((D, Q), jnp.float32)
    summed, unused = lax.scan(accumulate, start, (activations, cotangents, identifiers))
    fisher = summed / SEQS
    blocked = fisher.reshape(ROW_BLOCKS, ROW_SPAN, COL_BLOCKS, COL_SPAN).transpose(0, 2, 1, 3)
    return blocked.reshape(BLOCKS, ROW_SPAN, COL_SPAN) + damping

def reference(inputs, cotangent, token_ids, weights):
    damped = lax.map(one_model, (inputs, cotangent, token_ids))
    return lax.optimization_barrier(jnp.sum(damped * weights, axis=0)) / lax.optimization_barrier(jnp.sum(damped, axis=0))
```

```python
import jax
import jax.numpy as jnp
from jax import lax
from jax.experimental import pallas as pl
from jax.experimental.pallas import tpu as pltpu
from jax.sharding import PartitionSpec as P

FIRST_TEXT = 37984
DAMPING = 0.1
SUBS = 4
MESH = pl.DeviceIdType.MESH
Y_PEERS = ((1, 0), (3, 0), (1, 1), (3, 1), (2, 0), (2, 1), (0, 1))


def kernel(
    xt_ref, g_ref, w_ref, out_ref,
    rows, cols, fisher, chain, total, parts, wparts, sums, far, merged,
    row_s, row_r, col_s, col_r, chain_s, chain_r,
    w_s, w_r, part_s, part_r, far_s, far_r, out_s, out_r,
):
    mp = lax.axis_index("mp")
    tok = lax.axis_index("tok")
    x, zh = mp // 2, mp % 2
    y, z, c = tok // 16, (tok // 2) % 8, tok % 2
    me = y * 2 + c
    seq = xt_ref.shape[1]
    width = fisher.shape[2]
    height = fisher.shape[1]
    piece = height // SUBS
    band = piece // 4

    def at_y(dy, dc):
        there = (y + dy) % 4
        core = 1 - c if dc else c
        return there, core, (mp, (there * 8 + z) * 2 + core)

    def at_x(dx):
        there = (x + dx) % 4
        return there, (there * 2 + zh, tok)

    def at_z(dz):
        deep = zh * 8 + z + dz + 16
        return (x * 2 + (deep // 8) % 2, (y * 8 + deep % 8) * 2 + c)

    barrier = pltpu.get_barrier_semaphore()
    for dy, dc in Y_PEERS:
        pl.semaphore_signal(barrier, 1, device_id=at_y(dy, dc)[2], device_id_type=MESH)
    for dx in (1, 2, 3):
        pl.semaphore_signal(barrier, 1, device_id=at_x(dx)[1], device_id_type=MESH)
    for dz in (1, -1, 8):
        pl.semaphore_signal(barrier, 1, device_id=at_z(dz), device_id_type=MESH)
    pl.semaphore_wait(barrier, len(Y_PEERS) + 6)

    low = z < 4

    def k_of(i):
        return jnp.where(low, 3 - i, i)

    def row_copy(dy, dc, owner):
        there, core, device = at_y(dy, dc)
        slot = there * 2 + core if owner else me
        return pltpu.make_async_remote_copy(
            src_ref=xt_ref.at[pl.ds(there * 2 * height, 2 * height)],
            dst_ref=rows.at[slot],
            send_sem=row_s.at[there * 2 + core],
            recv_sem=row_r.at[slot],
            device_id=device,
            device_id_type=MESH,
        )

    def col_copy(k, dy, dc, owner):
        there, core, device = at_y(dy, dc)
        slot = there * 2 + core if owner else me
        return pltpu.make_async_remote_copy(
            src_ref=g_ref.at[:, pl.ds(pl.multiple_of((2 * k + core) * width, width), width)],
            dst_ref=cols.at[slot, k],
            send_sem=col_s.at[k, there * 2 + core],
            recv_sem=col_r.at[k, slot],
            device_id=device,
            device_id_type=MESH,
        )

    def w_copy(dx, owner):
        there, device = at_x(dx)
        slot = there if owner else x
        return pltpu.make_async_remote_copy(
            src_ref=w_ref.at[:, there],
            dst_ref=wparts.at[slot],
            send_sem=w_s.at[there],
            recv_sem=w_r.at[slot],
            device_id=device,
            device_id_type=MESH,
        )

    for dy, dc in Y_PEERS:
        row_copy(dy, dc, False).start()

    @pl.loop(0, 4)
    def _(i):
        for dy, dc in Y_PEERS:
            col_copy(k_of(i), dy, dc, False).start()

    for dx in (1, 2, 3):
        w_copy(dx, False).start()

    rows[me] = xt_ref[pl.ds(y * 2 * height, 2 * height), :]
    for k in range(4):
        cols[me, k] = g_ref[:, pl.ds(pl.multiple_of((2 * k + c) * width, width), width)]
    wparts[x] = w_ref[:, x]

    fisher[...] = jnp.zeros_like(fisher)

    for dy, dc in Y_PEERS:
        row_copy(dy, dc, True).wait_recv()

    def compute(i):
        k = k_of(i)
        for dy, dc in Y_PEERS:
            col_copy(k, dy, dc, True).wait_recv()

        @pl.loop(0, 8)
        def _(slot):
            right = cols[slot, k]
            for h in range(2):
                left = rows[slot, h * height:(h + 1) * height, :]
                gradient = jnp.dot(left, right, preferred_element_type=jnp.float32)
                fisher[4 * h + k] += gradient * gradient

    def chain_copy(way, d, s, source):
        span = pl.ds(s * piece, piece)
        return pltpu.make_async_remote_copy(
            src_ref=source.at[span],
            dst_ref=chain.at[way, d, span],
            send_sem=chain_s.at[way, d, s],
            recv_sem=chain_r.at[way, d, s],
            device_id=at_z(1 - 2 * way),
            device_id_type=MESH,
        )

    def chain_step(way, d):
        ahead = (d - z) * (1 - 2 * way)
        first = z == 7 * way

        @pl.when(jnp.logical_and(first, ahead > 0))
        def _():
            for s in range(SUBS):
                chain_copy(way, d, s, fisher.at[d]).start()

        @pl.when(jnp.logical_and(jnp.logical_not(first), ahead > 0))
        def _():
            for s in range(SUBS):
                span = slice(s * piece, (s + 1) * piece)
                chain_copy(way, d, s, chain.at[way, d]).wait_recv()
                chain[way, d, span] += fisher[d, span]
                chain_copy(way, d, s, chain.at[way, d]).start()

    main = jnp.where(low, 0, 1)
    place = jnp.where(low, z, 7 - z)

    def flip(d):
        return jnp.where(low, d, 7 - d)

    for i in range(4):
        compute(i)

        @pl.when(place == 0)
        def _():
            chain_step(main, flip(7 - i))

        if i > 0:
            @pl.when(place > 0)
            def _():
                chain_step(main, flip(8 - i))

    @pl.when(place > 0)
    def _():
        chain_step(main, flip(4))

    for i in range(3):
        chain_step(1 - main, flip(i))
        chain_step(main, flip(3 - i))

    def part_copy(s, dx, owner):
        there, device = at_x(dx)
        slot = there if owner else x
        return pltpu.make_async_remote_copy(
            src_ref=total.at[s, there],
            dst_ref=parts.at[s, slot],
            send_sem=part_s.at[s, there],
            recv_sem=part_r.at[s, slot],
            device_id=device,
            device_id_type=MESH,
        )

    def far_copy(s):
        return pltpu.make_async_remote_copy(
            src_ref=sums.at[s],
            dst_ref=far.at[s],
            send_sem=far_s.at[s],
            recv_sem=far_r.at[s],
            device_id=at_z(8),
            device_id_type=MESH,
        )

    def out_copy(s, dx, owner):
        there, device = at_x(dx)
        slot = there if owner else x
        return pltpu.make_async_remote_copy(
            src_ref=merged.at[s, slot],
            dst_ref=merged.at[s, slot],
            send_sem=out_s.at[s, there],
            recv_sem=out_r.at[s, slot],
            device_id=device,
            device_id_type=MESH,
        )

    scale = 1.0 / (seq * 64)
    for s in range(SUBS):
        span = slice(s * piece, (s + 1) * piece)
        for q in range(4):
            total[s, q] = fisher[z, s * piece + q * band:s * piece + (q + 1) * band]
        for way in (0, 1):
            @pl.when(z != 7 * way)
            def _():
                chain_copy(way, z, s, chain.at[way, z]).wait_recv()
                for q in range(4):
                    total[s, q] += chain[way, z, s * piece + q * band:s * piece + (q + 1) * band]
        for dx in (1, 2, 3):
            part_copy(s, dx, False).start()
        parts[s, x] = total[s, x]

    for dx in (1, 2, 3):
        w_copy(dx, True).wait_recv()
    for s in range(SUBS):
        for dx in (1, 2, 3):
            part_copy(s, dx, True).wait_recv()
        damped = [parts[s, m] * scale + DAMPING for m in range(4)]
        product = [damped[m] * wparts[m, s] for m in range(4)]
        sums[s, 0] = (product[0] + product[1]) + (product[2] + product[3])
        sums[s, 1] = (damped[0] + damped[1]) + (damped[2] + damped[3])
        far_copy(s).start()
    for s in range(SUBS):
        far_copy(s).wait_recv()
        merged[s, x] = (sums[s, 0] + far[s, 0]) / (sums[s, 1] + far[s, 1])
        for dx in (1, 2, 3):
            out_copy(s, dx, False).start()
    for s in range(SUBS):
        for dx in (1, 2, 3):
            out_copy(s, dx, True).wait_recv()
    out_ref[...] = merged[...]

    for dy, dc in Y_PEERS:
        row_copy(dy, dc, False).wait_send()

    @pl.loop(0, 4)
    def _(k):
        for dy, dc in Y_PEERS:
            col_copy(k, dy, dc, False).wait_send()

    for dx in (1, 2, 3):
        w_copy(dx, False).wait_send()
        for s in range(SUBS):
            part_copy(s, dx, False).wait_send()
            out_copy(s, dx, False).wait_send()
    for s in range(SUBS):
        far_copy(s).wait_send()

    @pl.loop(0, 8)
    def _(d):
        for way in (0, 1):
            @pl.when((d - z) * (1 - 2 * way) > 0)
            def _():
                for s in range(SUBS):
                    chain_copy(way, d, s, fisher.at[d]).wait_send()


def shards(inputs, cotangent, token_ids, weights):
    seq, feature = inputs.shape[2:]
    query = cotangent.shape[3]
    height, width = weights.shape[2:]
    band = height // SUBS // 4
    kept = (token_ids[0, 0] >= FIRST_TEXT).astype(jnp.bfloat16)
    turned = (inputs[0, 0] * kept[:, None]).T
    blocks = weights[0, 0].reshape(SUBS, 4, band, width)
    vmem = pl.BlockSpec(memory_space=pltpu.VMEM)
    dma = pltpu.SemaphoreType.DMA
    merged = pl.pallas_call(
        kernel,
        out_shape=jax.ShapeDtypeStruct((SUBS, 4, band, width), jnp.float32),
        in_specs=[vmem] * 3,
        out_specs=vmem,
        scratch_shapes=[
            pltpu.VMEM((8, 2 * height, seq), jnp.bfloat16),
            pltpu.VMEM((8, 4, seq, width), jnp.bfloat16),
            pltpu.VMEM((8, height, width), jnp.float32),
            pltpu.VMEM((2, 8, height, width), jnp.float32),
            pltpu.VMEM((SUBS, 4, band, width), jnp.float32),
            pltpu.VMEM((SUBS, 4, band, width), jnp.float32),
            pltpu.VMEM((4, SUBS, band, width), jnp.float32),
            pltpu.VMEM((SUBS, 2, band, width), jnp.float32),
            pltpu.VMEM((SUBS, 2, band, width), jnp.float32),
            pltpu.VMEM((SUBS, 4, band, width), jnp.float32),
            dma((8,)), dma((8,)), dma((4, 8)), dma((4, 8)),
            dma((2, 8, SUBS)), dma((2, 8, SUBS)),
            dma((4,)), dma((4,)), dma((SUBS, 4)), dma((SUBS, 4)),
            dma((SUBS,)), dma((SUBS,)), dma((SUBS, 4)), dma((SUBS, 4)),
        ],
        compiler_params=pltpu.CompilerParams(
            collective_id=0, has_side_effects=True, vmem_limit_bytes=48 * 1024 * 1024
        ),
    )(turned, cotangent[0, 0], blocks)
    return merged.reshape(1, height, width)


def solution(mesh):
    in_specs = (
        P("mp", "tok", None, None),
        P("mp", "tok", None, None),
        P("mp", "tok", None),
        P("mp", "tok", None, None),
    )
    out_specs = P("tok", None, None)
    return jax.shard_map(shards, mesh=mesh, in_specs=in_specs, out_specs=out_specs, check_vma=False)
```

```python
import jax
import jax.numpy as jnp
from jax import lax
from jax.experimental import pallas as pl
from jax.experimental.pallas import tpu as pltpu
from jax.sharding import PartitionSpec as P

FIRST_TEXT = 37984
DAMPING = 0.1
SUBS = 4
MESH = pl.DeviceIdType.MESH
Y_PEERS = ((1, 0), (3, 0), (1, 1), (3, 1), (2, 0), (2, 1), (0, 1))
OFFSET = DAMPING / 2
SHIFT = 1.0 / 64


def encode(values):
    root = values * SHIFT
    square = root * root
    fourth = square * square
    return (fourth * fourth).astype(jnp.bfloat16)


def decode(coded):
    inverse = lax.rsqrt(coded.astype(jnp.float32))
    square = lax.rsqrt(inverse)
    return square * lax.rsqrt(square) * (1.0 / SHIFT)


def kernel(
    xt_ref, g_ref, w_ref, out_ref,
    rows, cols, fisher, coded, chain, total, parts, wparts, sums, far, merged,
    row_s, row_r, col_s, col_r, coded_s, coded_r, chain_s, chain_r,
    w_s, w_r, part_s, part_r, far_s, far_r, out_s, out_r,
):
    mp = lax.axis_index("mp")
    tok = lax.axis_index("tok")
    x, zh = mp // 2, mp % 2
    y, z, c = tok // 16, (tok // 2) % 8, tok % 2
    me = y * 2 + c
    seq = xt_ref.shape[1]
    width = fisher.shape[2]
    height = fisher.shape[1]
    piece = height // SUBS
    band = piece // 4

    def at_y(dy, dc):
        there = (y + dy) % 4
        core = 1 - c if dc else c
        return there, core, (mp, (there * 8 + z) * 2 + core)

    def at_x(dx):
        there = (x + dx) % 4
        return there, (there * 2 + zh, tok)

    def at_z(dz):
        deep = zh * 8 + z + dz + 16
        return (x * 2 + (deep // 8) % 2, (y * 8 + deep % 8) * 2 + c)

    barrier = pltpu.get_barrier_semaphore()
    for dy, dc in Y_PEERS:
        pl.semaphore_signal(barrier, 1, device_id=at_y(dy, dc)[2], device_id_type=MESH)
    for dx in (1, 2, 3):
        pl.semaphore_signal(barrier, 1, device_id=at_x(dx)[1], device_id_type=MESH)
    for dz in (1, -1, 8):
        pl.semaphore_signal(barrier, 1, device_id=at_z(dz), device_id_type=MESH)
    pl.semaphore_wait(barrier, len(Y_PEERS) + 6)

    low = z < 4

    def k_of(i):
        return jnp.where(low, 3 - i, i)

    def row_copy(dy, dc, owner):
        there, core, device = at_y(dy, dc)
        slot = there * 2 + core if owner else me
        return pltpu.make_async_remote_copy(
            src_ref=xt_ref.at[pl.ds(there * 2 * height, 2 * height)],
            dst_ref=rows.at[slot],
            send_sem=row_s.at[there * 2 + core],
            recv_sem=row_r.at[slot],
            device_id=device,
            device_id_type=MESH,
        )

    def row_pass(dy, owner):
        there = (y + dy) % 4
        slot = there * 2 + (1 - c if owner else c)
        return pltpu.make_async_remote_copy(
            src_ref=rows.at[slot],
            dst_ref=rows.at[slot],
            send_sem=row_s.at[there * 2 + 1 - c],
            recv_sem=row_r.at[slot],
            device_id=at_y(0, 1)[2],
            device_id_type=MESH,
        )

    def col_copy(k, dy, dc):
        there, core, device = at_y(dy, dc)
        return pltpu.make_async_remote_copy(
            src_ref=g_ref.at[:, pl.ds(pl.multiple_of((2 * k + core) * width, width), width)],
            dst_ref=cols.at[me, k],
            send_sem=col_s.at[k, there * 2 + core],
            recv_sem=col_r.at[k, me],
            device_id=device,
            device_id_type=MESH,
        )

    def col_wait(k, slot):
        pltpu.make_async_remote_copy(
            src_ref=cols.at[slot, k],
            dst_ref=cols.at[slot, k],
            send_sem=col_s.at[k, slot],
            recv_sem=col_r.at[k, slot],
            device_id=at_y(0, 1)[2],
            device_id_type=MESH,
        ).wait_recv()

    def col_pass(k, core):
        step = 1 - 2 * core
        slot = ((y + 4 - step) % 4) * 2 + core
        return pltpu.make_async_remote_copy(
            src_ref=cols.at[slot, k],
            dst_ref=cols.at[slot, k],
            send_sem=col_s.at[k, ((y + 2) % 4) * 2 + core],
            recv_sem=col_r.at[k, slot],
            device_id=at_y(step + 4, 0)[2],
            device_id_type=MESH,
        )

    def w_copy(dx, owner):
        there, device = at_x(dx)
        slot = there if owner else x
        return pltpu.make_async_remote_copy(
            src_ref=w_ref.at[:, there],
            dst_ref=wparts.at[slot],
            send_sem=w_s.at[there],
            recv_sem=w_r.at[slot],
            device_id=device,
            device_id_type=MESH,
        )

    def send(i):
        for dy, dc in ((1, 0), (3, 0), (1, 1), (3, 1), (0, 1)):
            col_copy(k_of(i), dy, dc).start()

    def forward(i):
        for core in (0, 1):
            slot = ((y + 3 + 2 * core) % 4) * 2 + core
            col_wait(k_of(i), slot)
            col_pass(k_of(i), core).start()

    for dy, dc in ((1, 0), (3, 0), (2, 0), (0, 1)):
        row_copy(dy, dc, False).start()
    send(0)
    send(1)
    for dx in (1, 2, 3):
        w_copy(dx, False).start()

    rows[me] = xt_ref[pl.ds(y * 2 * height, 2 * height), :]
    for k in range(4):
        cols[me, k] = g_ref[:, pl.ds(pl.multiple_of((2 * k + c) * width, width), width)]
    wparts[x] = w_ref[:, x]
    fisher[...] = jnp.zeros_like(fisher)

    for dy in (1, 3, 2):
        row_copy(dy, 0, True).wait_recv()
        row_pass(dy, False).start()
    forward(0)
    send(2)
    row_copy(0, 1, True).wait_recv()
    for dy in (1, 3, 2):
        row_pass(dy, True).wait_recv()

    def compute(i):
        k = k_of(i)
        for slot in (((y + 3) % 4) * 2 + 1, ((y + 1) % 4) * 2, y * 2 + 1 - c, ((y + 2) % 4) * 2, ((y + 2) % 4) * 2 + 1):
            col_wait(k, slot)

        @pl.loop(0, 8)
        def _(slot):
            right = cols[slot, k]
            for h in range(2):
                left = rows[slot, h * height:(h + 1) * height, :]
                gradient = jnp.dot(left, right, preferred_element_type=jnp.float32)
                fisher[4 * h + k] += gradient * gradient

    scale = 1.0 / (seq * 64)
    main = jnp.where(low, 0, 1)
    place = jnp.where(low, z, 7 - z)

    def flip(d):
        return jnp.where(low, d, 7 - d)

    def coded_copy(way, d, s):
        span = pl.ds(s * piece, piece)
        return pltpu.make_async_remote_copy(
            src_ref=coded.at[way, d, span],
            dst_ref=coded.at[way, d, span],
            send_sem=coded_s.at[way, d, s],
            recv_sem=coded_r.at[way, d, s],
            device_id=at_z(1 - 2 * way),
            device_id_type=MESH,
        )

    def chain_copy(way, d, s):
        span = pl.ds(s * piece, piece)
        return pltpu.make_async_remote_copy(
            src_ref=chain.at[way, d, span],
            dst_ref=chain.at[way, d, span],
            send_sem=chain_s.at[way, d, s],
            recv_sem=chain_r.at[way, d, s],
            device_id=at_z(1 - 2 * way),
            device_id_type=MESH,
        )

    def main_step(away):
        d = flip(away)

        @pl.when(place == 0)
        def _():
            for s in range(SUBS):
                span = slice(s * piece, (s + 1) * piece)
                coded[main, d, span] = encode(fisher[d, span] * scale + OFFSET)
                coded_copy(main, d, s).start()

        @pl.when(jnp.logical_and(place > 0, place < away))
        def _():
            for s in range(SUBS):
                span = slice(s * piece, (s + 1) * piece)
                coded_copy(main, d, s).wait_recv()
                coded[main, d, span] = encode(decode(coded[main, d, span]) + fisher[d, span] * scale)
                coded_copy(main, d, s).start()

    def back_step(away):
        d = flip(away)

        @pl.when(place == 3)
        def _():
            for s in range(SUBS):
                span = slice(s * piece, (s + 1) * piece)
                coded_copy(1 - main, d, s).wait_recv()
                chain[1 - main, d, span] = decode(coded[1 - main, d, span]) + fisher[d, span] * scale
                chain_copy(1 - main, d, s).start()

        @pl.when(jnp.logical_and(place < 3, place > away))
        def _():
            for s in range(SUBS):
                span = slice(s * piece, (s + 1) * piece)
                chain_copy(1 - main, d, s).wait_recv()
                chain[1 - main, d, span] += fisher[d, span] * scale
                chain_copy(1 - main, d, s).start()

    def end_steps(*away):
        @pl.when(place == 0)
        def _():
            for one in away:
                main_step(one)

    def inner_steps(*away):
        @pl.when(place > 0)
        def _():
            for one in away:
                main_step(one)

    forward(1)
    send(3)
    compute(0)
    end_steps(7, 3)
    forward(2)
    compute(1)
    end_steps(6)
    inner_steps(7)
    forward(3)
    compute(2)
    end_steps(5)
    inner_steps(3)
    compute(3)
    end_steps(4, 2, 1)
    inner_steps(6)

    @pl.when(place > 1)
    def _():
        back_step(0)

    inner_steps(5)

    @pl.when(place == 1)
    def _():
        back_step(0)

    back_step(1)
    inner_steps(4)
    back_step(2)
    inner_steps(2)

    def part_copy(s, dx, owner):
        there, device = at_x(dx)
        slot = there if owner else x
        return pltpu.make_async_remote_copy(
            src_ref=total.at[s, there],
            dst_ref=parts.at[s, slot],
            send_sem=part_s.at[s, there],
            recv_sem=part_r.at[s, slot],
            device_id=device,
            device_id_type=MESH,
        )

    def far_copy(s):
        return pltpu.make_async_remote_copy(
            src_ref=sums.at[s],
            dst_ref=far.at[s],
            send_sem=far_s.at[s],
            recv_sem=far_r.at[s],
            device_id=at_z(8),
            device_id_type=MESH,
        )

    def out_copy(s, dx, owner):
        there, device = at_x(dx)
        slot = there if owner else x
        return pltpu.make_async_remote_copy(
            src_ref=merged.at[s, slot],
            dst_ref=merged.at[s, slot],
            send_sem=out_s.at[s, there],
            recv_sem=out_r.at[s, slot],
            device_id=device,
            device_id_type=MESH,
        )

    for s in range(SUBS):
        base = s * piece

        @pl.when(place == 0)
        def _():
            chain_copy(1 - main, z, s).wait_recv()
            for q in range(4):
                span = slice(base + q * band, base + (q + 1) * band)
                total[s, q] = fisher[z, span] * scale + OFFSET + chain[1 - main, z, span]

        @pl.when(jnp.logical_and(place > 0, place < 3))
        def _():
            coded_copy(main, z, s).wait_recv()
            chain_copy(1 - main, z, s).wait_recv()
            for q in range(4):
                span = slice(base + q * band, base + (q + 1) * band)
                total[s, q] = fisher[z, span] * scale + decode(coded[main, z, span]) + chain[1 - main, z, span]

        @pl.when(place == 3)
        def _():
            coded_copy(main, z, s).wait_recv()
            coded_copy(1 - main, z, s).wait_recv()
            for q in range(4):
                span = slice(base + q * band, base + (q + 1) * band)
                total[s, q] = (
                    fisher[z, span] * scale + decode(coded[main, z, span]) + decode(coded[1 - main, z, span])
                )

        for dx in (1, 2, 3):
            part_copy(s, dx, False).start()
        parts[s, x] = total[s, x]

    for dx in (1, 2, 3):
        w_copy(dx, True).wait_recv()
    for s in range(SUBS):
        for dx in (1, 2, 3):
            part_copy(s, dx, True).wait_recv()
        damped = [parts[s, m] for m in range(4)]
        product = [damped[m] * wparts[m, s] for m in range(4)]
        sums[s, 0] = (product[0] + product[1]) + (product[2] + product[3])
        sums[s, 1] = (damped[0] + damped[1]) + (damped[2] + damped[3])
        far_copy(s).start()
    for s in range(SUBS):
        far_copy(s).wait_recv()
        merged[s, x] = (sums[s, 0] + far[s, 0]) / (sums[s, 1] + far[s, 1])
        for dx in (1, 2, 3):
            out_copy(s, dx, False).start()
    for s in range(SUBS):
        for dx in (1, 2, 3):
            out_copy(s, dx, True).wait_recv()
    out_ref[...] = merged[...]

    for dy, dc in ((1, 0), (3, 0), (2, 0), (0, 1)):
        row_copy(dy, dc, False).wait_send()
    for dy in (1, 3, 2):
        row_pass(dy, False).wait_send()

    @pl.loop(0, 4)
    def _(k):
        for dy, dc in ((1, 0), (3, 0), (1, 1), (3, 1), (0, 1)):
            col_copy(k, dy, dc).wait_send()
        for core in (0, 1):
            col_pass(k, core).wait_send()

    for dx in (1, 2, 3):
        w_copy(dx, False).wait_send()
        for s in range(SUBS):
            part_copy(s, dx, False).wait_send()
            out_copy(s, dx, False).wait_send()
    for s in range(SUBS):
        far_copy(s).wait_send()

    @pl.loop(0, 8)
    def _(away):
        @pl.when(away > place)
        def _():
            for s in range(SUBS):
                coded_copy(main, flip(away), s).wait_send()

        @pl.when(away < place)
        def _():
            for s in range(SUBS):
                chain_copy(1 - main, flip(away), s).wait_send()


def shards(inputs, cotangent, token_ids, weights):
    seq, feature = inputs.shape[2:]
    query = cotangent.shape[3]
    height, width = weights.shape[2:]
    band = height // SUBS // 4
    kept = (token_ids[0, 0] >= FIRST_TEXT).astype(jnp.bfloat16)
    turned = (inputs[0, 0] * kept[:, None]).T
    blocks = weights[0, 0].reshape(SUBS, 4, band, width)
    vmem = pl.BlockSpec(memory_space=pltpu.VMEM)
    dma = pltpu.SemaphoreType.DMA
    merged = pl.pallas_call(
        kernel,
        out_shape=jax.ShapeDtypeStruct((SUBS, 4, band, width), jnp.float32),
        in_specs=[vmem] * 3,
        out_specs=vmem,
        scratch_shapes=[
            pltpu.VMEM((8, 2 * height, seq), jnp.bfloat16),
            pltpu.VMEM((8, 4, seq, width), jnp.bfloat16),
            pltpu.VMEM((8, height, width), jnp.float32),
            pltpu.VMEM((2, 8, height, width), jnp.bfloat16),
            pltpu.VMEM((2, 8, height, width), jnp.float32),
            pltpu.VMEM((SUBS, 4, band, width), jnp.float32),
            pltpu.VMEM((SUBS, 4, band, width), jnp.float32),
            pltpu.VMEM((4, SUBS, band, width), jnp.float32),
            pltpu.VMEM((SUBS, 2, band, width), jnp.float32),
            pltpu.VMEM((SUBS, 2, band, width), jnp.float32),
            pltpu.VMEM((SUBS, 4, band, width), jnp.float32),
            dma((8,)), dma((8,)), dma((4, 8)), dma((4, 8)),
            dma((2, 8, SUBS)), dma((2, 8, SUBS)), dma((2, 8, SUBS)), dma((2, 8, SUBS)),
            dma((4,)), dma((4,)), dma((SUBS, 4)), dma((SUBS, 4)),
            dma((SUBS,)), dma((SUBS,)), dma((SUBS, 4)), dma((SUBS, 4)),
        ],
        compiler_params=pltpu.CompilerParams(
            collective_id=0, has_side_effects=True, vmem_limit_bytes=48 * 1024 * 1024
        ),
    )(turned, cotangent[0, 0], blocks)
    return merged.reshape(1, height, width)


def solution(mesh):
    in_specs = (
        P("mp", "tok", None, None),
        P("mp", "tok", None, None),
        P("mp", "tok", None),
        P("mp", "tok", None, None),
    )
    out_specs = P("tok", None, None)
    return jax.shard_map(shards, mesh=mesh, in_specs=in_specs, out_specs=out_specs, check_vma=False)
```

```python
import jax
import jax.numpy as jnp
from jax import lax
from jax.experimental import pallas as pl
from jax.experimental.pallas import tpu as pltpu
from jax.sharding import PartitionSpec as P

FIRST_TEXT = 37984
DAMPING = 0.1
SUBS = 4
MESH = pl.DeviceIdType.MESH
Y_PEERS = ((1, 0), (3, 0), (1, 1), (3, 1), (2, 0), (2, 1), (0, 1))
OFFSET = DAMPING / 2
MIDDLE = 90.5
LOW_UNIT = 2.0
HIGH_UNIT = 4096.0


def encode(values):
    small = values < MIDDLE
    ratio = values * jnp.where(small, 1.0 / LOW_UNIT, 1.0 / HIGH_UNIT)
    square = ratio * ratio
    fourth = square * square
    eighth = fourth * fourth
    power = (eighth * eighth) * (fourth * square)
    return jnp.where(small, power, -power).astype(jnp.bfloat16)


def decode(code):
    power = code.astype(jnp.float32)
    ratio = jnp.exp2(jnp.log2(jnp.abs(power)) * (1.0 / 22))
    return ratio * jnp.where(power > 0, LOW_UNIT, HIGH_UNIT)


def kernel(
    xt_ref, g_hbm, w_hbm, out_ref,
    g_ref, w_ref, rows, cols, fisher, coded, total, parts, wparts,
    tops, bottoms, far_tops, far_bottoms, merged, load_s,
    row_s, row_r, col_s, col_r, coded_s, coded_r,
    w_s, w_r, part_s, part_r, far_s, far_r, out_s, out_r,
):
    loads = (
        pltpu.make_async_copy(g_hbm, g_ref, load_s.at[0]),
        pltpu.make_async_copy(w_hbm, w_ref, load_s.at[1]),
    )
    for load in loads:
        load.start()
    mp = lax.axis_index("mp")
    tok = lax.axis_index("tok")
    x, zh = mp // 2, mp % 2
    y, z, c = tok // 16, (tok // 2) % 8, tok % 2
    me = y * 2 + c
    seq = xt_ref.shape[1]
    width = fisher.shape[2]
    height = fisher.shape[1]
    piece = height // SUBS
    band = piece // 4

    def at_y(dy, dc):
        there = (y + dy) % 4
        core = 1 - c if dc else c
        return there, core, (mp, (there * 8 + z) * 2 + core)

    def at_x(dx):
        there = (x + dx) % 4
        return there, (there * 2 + zh, tok)

    def at_z(dz):
        deep = zh * 8 + z + dz + 16
        return (x * 2 + (deep // 8) % 2, (y * 8 + deep % 8) * 2 + c)

    barrier = pltpu.get_barrier_semaphore()
    for dy, dc in Y_PEERS:
        pl.semaphore_signal(barrier, 1, device_id=at_y(dy, dc)[2], device_id_type=MESH)
    for dx in (1, 2, 3):
        pl.semaphore_signal(barrier, 1, device_id=at_x(dx)[1], device_id_type=MESH)
    for dz in (1, -1, 8):
        pl.semaphore_signal(barrier, 1, device_id=at_z(dz), device_id_type=MESH)
    pl.semaphore_wait(barrier, len(Y_PEERS) + 6)

    for load in loads:
        load.wait()

    low = z < 4

    def k_of(i):
        return jnp.where(low, 3 - i, i)

    def row_copy(dy, dc, owner):
        there, core, device = at_y(dy, dc)
        slot = there * 2 + core if owner else me
        return pltpu.make_async_remote_copy(
            src_ref=xt_ref.at[pl.ds(there * 2 * height, 2 * height)],
            dst_ref=rows.at[slot],
            send_sem=row_s.at[there * 2 + core],
            recv_sem=row_r.at[slot],
            device_id=device,
            device_id_type=MESH,
        )

    def row_pass(dy, owner):
        there = (y + dy) % 4
        slot = there * 2 + (1 - c if owner else c)
        return pltpu.make_async_remote_copy(
            src_ref=rows.at[slot],
            dst_ref=rows.at[slot],
            send_sem=row_s.at[there * 2 + 1 - c],
            recv_sem=row_r.at[slot],
            device_id=at_y(0, 1)[2],
            device_id_type=MESH,
        )

    def col_copy(k, dy, dc):
        there, core, device = at_y(dy, dc)
        return pltpu.make_async_remote_copy(
            src_ref=g_ref.at[:, pl.ds(pl.multiple_of((2 * k + core) * width, width), width)],
            dst_ref=cols.at[me, k],
            send_sem=col_s.at[k, there * 2 + core],
            recv_sem=col_r.at[k, me],
            device_id=device,
            device_id_type=MESH,
        )

    def col_wait(k, slot):
        pltpu.make_async_remote_copy(
            src_ref=cols.at[slot, k],
            dst_ref=cols.at[slot, k],
            send_sem=col_s.at[k, slot],
            recv_sem=col_r.at[k, slot],
            device_id=at_y(0, 1)[2],
            device_id_type=MESH,
        ).wait_recv()

    def col_pass(k, core):
        step = 1 - 2 * core
        slot = ((y + 4 - step) % 4) * 2 + core
        return pltpu.make_async_remote_copy(
            src_ref=cols.at[slot, k],
            dst_ref=cols.at[slot, k],
            send_sem=col_s.at[k, ((y + 2) % 4) * 2 + core],
            recv_sem=col_r.at[k, slot],
            device_id=at_y(step + 4, 0)[2],
            device_id_type=MESH,
        )

    def w_copy(dx, owner):
        there, device = at_x(dx)
        slot = there if owner else x
        return pltpu.make_async_remote_copy(
            src_ref=w_ref.at[:, there],
            dst_ref=wparts.at[slot],
            send_sem=w_s.at[there],
            recv_sem=w_r.at[slot],
            device_id=device,
            device_id_type=MESH,
        )

    def send(i):
        for back in (0, 1):
            for dc in (0, 1):
                col_copy(k_of(i), 1 + 2 * ((c + back) % 2), dc).start()
        col_copy(k_of(i), 0, 1).start()

    def forward(i):
        for core in (0, 1):
            slot = ((y + 3 + 2 * core) % 4) * 2 + core
            col_wait(k_of(i), slot)
            col_pass(k_of(i), core).start()

    for dy, dc in ((1, 0), (3, 0), (2, 0), (0, 1)):
        row_copy(dy, dc, False).start()
    send(0)
    for dx in (1, 2, 3):
        w_copy(dx, False).start()

    rows[me] = xt_ref[pl.ds(y * 2 * height, 2 * height), :]
    for k in range(4):
        cols[me, k] = g_ref[:, pl.ds(pl.multiple_of((2 * k + c) * width, width), width)]
    wparts[x] = w_ref[:, x]
    fisher[...] = jnp.zeros_like(fisher)

    for dy in (1, 3, 2):
        row_copy(dy, 0, True).wait_recv()
        row_pass(dy, False).start()
    forward(0)
    send(1)
    row_copy(0, 1, True).wait_recv()
    for dy in (1, 3, 2):
        row_pass(dy, True).wait_recv()

    def compute(i):
        k = k_of(i)
        for slot in (((y + 3) % 4) * 2 + 1, ((y + 1) % 4) * 2, y * 2 + 1 - c, ((y + 2) % 4) * 2, ((y + 2) % 4) * 2 + 1):
            col_wait(k, slot)

        @pl.loop(0, 8)
        def _(slot):
            right = cols[slot, k]
            for h in range(2):
                left = rows[slot, h * height:(h + 1) * height, :]
                gradient = jnp.dot(left, right, preferred_element_type=jnp.float32)
                fisher[4 * h + k] += gradient * gradient

    scale = 1.0 / (seq * 64)
    main = jnp.where(low, 0, 1)
    place = jnp.where(low, z, 7 - z)

    def flip(d):
        return jnp.where(low, d, 7 - d)

    def coded_copy(way, d, s):
        span = pl.ds(s * piece, piece)
        return pltpu.make_async_remote_copy(
            src_ref=coded.at[way, d, span],
            dst_ref=coded.at[way, d, span],
            send_sem=coded_s.at[way, d, s],
            recv_sem=coded_r.at[way, d, s],
            device_id=at_z(1 - 2 * way),
            device_id_type=MESH,
        )

    def piece_of(s):
        return pl.ds(pl.multiple_of(s * piece, piece), piece)

    def first_step(away):
        d = flip(away)

        @pl.loop(0, SUBS)
        def _(s):
            coded[main, d, piece_of(s)] = encode(fisher[d, piece_of(s)] * scale + OFFSET)
            coded_copy(main, d, s).start()

    def step(way, away):
        d = flip(away)

        @pl.loop(0, SUBS)
        def _(s):
            coded_copy(way, d, s).wait_recv()
            own = fisher[d, piece_of(s)] * scale
            coded[way, d, piece_of(s)] = encode(decode(coded[way, d, piece_of(s)]) + own)
            coded_copy(way, d, s).start()

    def steps(where, *aways):
        @pl.when(place == where)
        def _():
            for away in aways:
                if where == 0:
                    first_step(away)
                elif away < 0:
                    step(1 - main, -away % 8)
                else:
                    step(main, away)

    compute(0)
    steps(0, 7, 3)
    forward(1)
    send(2)
    compute(1)
    steps(0, 6)
    forward(2)
    send(3)
    steps(1, 7, 3)
    steps(2, 7)
    compute(2)
    steps(0, 5)
    forward(3)
    steps(1, 6)
    steps(2, 3)
    steps(3, 7)
    compute(3)
    steps(0, 4, 2, 1)
    steps(1, 5, -8, 4, 2)
    steps(2, 6, -8, 5, -1, 4)
    steps(3, -8, 6, -1, 5, -2, 4)

    def part_copy(s, dx, owner):
        there, device = at_x(dx)
        slot = there if owner else x
        return pltpu.make_async_remote_copy(
            src_ref=total.at[s, there],
            dst_ref=parts.at[s, slot],
            send_sem=part_s.at[s, there],
            recv_sem=part_r.at[s, slot],
            device_id=device,
            device_id_type=MESH,
        )

    def far_copies(s):
        return [
            pltpu.make_async_remote_copy(
                src_ref=here.at[s],
                dst_ref=there.at[s],
                send_sem=far_s.at[kind, s],
                recv_sem=far_r.at[kind, s],
                device_id=at_z(8),
                device_id_type=MESH,
            )
            for kind, (here, there) in enumerate(((tops, far_tops), (bottoms, far_bottoms)))
        ]

    def out_copy(s, dx, owner):
        there, device = at_x(dx)
        slot = there if owner else x
        return pltpu.make_async_remote_copy(
            src_ref=merged.at[s, slot],
            dst_ref=merged.at[s, slot],
            send_sem=out_s.at[s, there],
            recv_sem=out_r.at[s, slot],
            device_id=device,
            device_id_type=MESH,
        )

    for s in range(SUBS):
        base = s * piece
        coded_copy(1 - main, z, s).wait_recv()

        @pl.when(place == 0)
        def _():
            for q in range(4):
                span = slice(base + q * band, base + (q + 1) * band)
                total[s, q] = fisher[z, span] * scale + OFFSET + decode(coded[1 - main, z, span])

        @pl.when(place > 0)
        def _():
            coded_copy(main, z, s).wait_recv()
            for q in range(4):
                span = slice(base + q * band, base + (q + 1) * band)
                total[s, q] = (
                    fisher[z, span] * scale + decode(coded[main, z, span]) + decode(coded[1 - main, z, span])
                )

        for dx in (1, 2, 3):
            part_copy(s, dx, False).start()
        parts[s, x] = total[s, x]

    for dx in (1, 2, 3):
        w_copy(dx, True).wait_recv()
    for s in range(SUBS):
        for dx in (1, 2, 3):
            part_copy(s, dx, True).wait_recv()
        damped = [parts[s, m] for m in range(4)]
        product = [damped[m] * wparts[m, s] for m in range(4)]
        tops[s] = (product[0] + product[1]) + (product[2] + product[3])
        bottoms[s] = encode(((damped[0] + damped[1]) + (damped[2] + damped[3])) * 0.25)
        for copy in far_copies(s):
            copy.start()
    for s in range(SUBS):
        for copy in far_copies(s):
            copy.wait_recv()
        bottom = decode(bottoms[s]) + decode(far_bottoms[s])
        merged[s, x] = (tops[s] + far_tops[s]) * 0.25 / bottom
        for dx in (1, 2, 3):
            out_copy(s, dx, False).start()
    for s in range(SUBS):
        for dx in (1, 2, 3):
            out_copy(s, dx, True).wait_recv()
    out_ref[...] = merged[...]

    for dy, dc in ((1, 0), (3, 0), (2, 0), (0, 1)):
        row_copy(dy, dc, False).wait_send()
    for dy in (1, 3, 2):
        row_pass(dy, False).wait_send()

    @pl.loop(0, 4)
    def _(k):
        for dy, dc in ((1, 0), (3, 0), (1, 1), (3, 1), (0, 1)):
            col_copy(k, dy, dc).wait_send()
        for core in (0, 1):
            col_pass(k, core).wait_send()

    for dx in (1, 2, 3):
        w_copy(dx, False).wait_send()
        for s in range(SUBS):
            part_copy(s, dx, False).wait_send()
            out_copy(s, dx, False).wait_send()
    for s in range(SUBS):
        for copy in far_copies(s):
            copy.wait_send()

    @pl.loop(0, 8)
    def _(away):
        @pl.when(away != place)
        def _():
            for s in range(SUBS):
                coded_copy(jnp.where(away > place, main, 1 - main), flip(away), s).wait_send()


def shards(inputs, cotangent, token_ids, weights):
    seq, feature = inputs.shape[2:]
    query = cotangent.shape[3]
    height, width = weights.shape[2:]
    band = height // SUBS // 4
    kept = (token_ids[0, 0] >= FIRST_TEXT).astype(jnp.bfloat16)
    turned = (inputs[0, 0] * kept[:, None]).T
    blocks = weights[0, 0].reshape(SUBS, 4, band, width)
    vmem = pl.BlockSpec(memory_space=pltpu.VMEM)
    dma = pltpu.SemaphoreType.DMA
    merged = pl.pallas_call(
        kernel,
        out_shape=jax.ShapeDtypeStruct((SUBS, 4, band, width), jnp.float32),
        in_specs=[vmem, pl.BlockSpec(memory_space=pl.ANY), pl.BlockSpec(memory_space=pl.ANY)],
        out_specs=vmem,
        scratch_shapes=[
            pltpu.VMEM((seq, query), jnp.bfloat16),
            pltpu.VMEM((SUBS, 4, band, width), jnp.float32),
            pltpu.VMEM((8, 2 * height, seq), jnp.bfloat16),
            pltpu.VMEM((8, 4, seq, width), jnp.bfloat16),
            pltpu.VMEM((8, height, width), jnp.float32),
            pltpu.VMEM((2, 8, height, width), jnp.bfloat16),
            pltpu.VMEM((SUBS, 4, band, width), jnp.float32),
            pltpu.VMEM((SUBS, 4, band, width), jnp.float32),
            pltpu.VMEM((4, SUBS, band, width), jnp.float32),
            pltpu.VMEM((SUBS, band, width), jnp.float32),
            pltpu.VMEM((SUBS, band, width), jnp.bfloat16),
            pltpu.VMEM((SUBS, band, width), jnp.float32),
            pltpu.VMEM((SUBS, band, width), jnp.bfloat16),
            pltpu.VMEM((SUBS, 4, band, width), jnp.float32),
            dma((2,)),
            dma((8,)), dma((8,)), dma((4, 8)), dma((4, 8)),
            dma((2, 8, SUBS)), dma((2, 8, SUBS)),
            dma((4,)), dma((4,)), dma((SUBS, 4)), dma((SUBS, 4)),
            dma((2, SUBS)), dma((2, SUBS)), dma((SUBS, 4)), dma((SUBS, 4)),
        ],
        compiler_params=pltpu.CompilerParams(
            collective_id=0, has_side_effects=True, vmem_limit_bytes=48 * 1024 * 1024
        ),
    )(turned, cotangent[0, 0], blocks)
    return merged.reshape(1, height, width)


def solution(mesh):
    in_specs = (
        P("mp", "tok", None, None),
        P("mp", "tok", None, None),
        P("mp", "tok", None),
        P("mp", "tok", None, None),
    )
    out_specs = P("tok", None, None)
    return jax.shard_map(shards, mesh=mesh, in_specs=in_specs, out_specs=out_specs, check_vma=False)
```

```python
import jax
import jax.numpy as jnp
from jax import lax
from jax.experimental import pallas as pl
from jax.experimental.pallas import tpu as pltpu
from jax.sharding import PartitionSpec as P

FIRST_TEXT = 37984
DAMPING = 0.1
ROUNDS = 2
SUBS = 2
MESH = pl.DeviceIdType.MESH
Y_PEERS = ((1, 0), (3, 0), (1, 1), (3, 1), (2, 0), (2, 1), (0, 1))
OFFSET = DAMPING / 2
MIDDLE = 90.5
LOW_UNIT = 2.0
HIGH_UNIT = 4096.0


def encode(values):
    small = values < MIDDLE
    ratio = values * jnp.where(small, 1.0 / LOW_UNIT, 1.0 / HIGH_UNIT)
    square = ratio * ratio
    fourth = square * square
    eighth = fourth * fourth
    power = (eighth * eighth) * (fourth * square)
    return jnp.where(small, power, -power).astype(jnp.bfloat16)


def decode(code):
    power = code.astype(jnp.float32)
    ratio = jnp.exp2(jnp.log2(jnp.abs(power)) * (1.0 / 22))
    return ratio * jnp.where(power > 0, LOW_UNIT, HIGH_UNIT)


def kernel(
    x_hbm, g_hbm, w_hbm, ids_ref, out_ref,
    x_ref, xt_ref, g_ref, w_ref, rows, cols, fisher, coded, total, parts, wparts,
    tops, bottoms, far_tops, far_bottoms, merged, load_s,
    row_s, row_r, col_s, col_r, coded_s, coded_r,
    w_s, w_r, part_s, part_r, far_s, far_r, out_s, out_r,
):
    loads = (
        pltpu.make_async_copy(x_hbm, x_ref, load_s.at[0]),
        pltpu.make_async_copy(g_hbm, g_ref, load_s.at[1]),
        pltpu.make_async_copy(w_hbm, w_ref, load_s.at[2]),
    )
    for load in loads:
        load.start()
    mp = lax.axis_index("mp")
    tok = lax.axis_index("tok")
    x, zh = mp // 2, mp % 2
    y, z, c = tok // 16, (tok // 2) % 8, tok % 2
    me = y * 2 + c
    seq = g_ref.shape[0]
    width = w_ref.shape[3]
    height, part = fisher.shape[1:]
    piece = height // SUBS
    band = piece // 4

    def at_y(dy, dc):
        there = (y + dy) % 4
        core = 1 - c if dc else c
        return there, core, (mp, (there * 8 + z) * 2 + core)

    def at_x(dx):
        there = (x + dx) % 4
        return there, (there * 2 + zh, tok)

    def at_z(dz):
        deep = zh * 8 + z + dz + 16
        return (x * 2 + (deep // 8) % 2, (y * 8 + deep % 8) * 2 + c)

    barrier = pltpu.get_barrier_semaphore()
    for dy, dc in Y_PEERS:
        pl.semaphore_signal(barrier, 1, device_id=at_y(dy, dc)[2], device_id_type=MESH)
    for dx in (1, 2, 3):
        pl.semaphore_signal(barrier, 1, device_id=at_x(dx)[1], device_id_type=MESH)
    for dz in (1, -1, 8):
        pl.semaphore_signal(barrier, 1, device_id=at_z(dz), device_id_type=MESH)
    loads[0].wait()
    kept = ids_ref[...] >= FIRST_TEXT
    for r in range(8):
        some = x_ref[:, r * height:(r + 1) * height].astype(jnp.float32).T
        xt_ref[r * height:(r + 1) * height, :] = jnp.where(kept, some, 0.0).astype(jnp.bfloat16)

    pl.semaphore_wait(barrier, len(Y_PEERS) + 6)

    for load in loads[1:]:
        load.wait()

    low = z < 4

    def unit_of(u):
        return u // 4 * 4 + jnp.where(low, 3 - u % 4, u % 4)

    def row_copy(dy, dc, owner):
        there, core, device = at_y(dy, dc)
        slot = there * 2 + core if owner else me
        return pltpu.make_async_remote_copy(
            src_ref=xt_ref.at[pl.ds(there * 2 * height, 2 * height)],
            dst_ref=rows.at[slot],
            send_sem=row_s.at[there * 2 + core],
            recv_sem=row_r.at[slot],
            device_id=device,
            device_id_type=MESH,
        )

    def row_pass(dy, owner):
        there = (y + dy) % 4
        slot = there * 2 + (1 - c if owner else c)
        return pltpu.make_async_remote_copy(
            src_ref=rows.at[slot],
            dst_ref=rows.at[slot],
            send_sem=row_s.at[there * 2 + 1 - c],
            recv_sem=row_r.at[slot],
            device_id=at_y(0, 1)[2],
            device_id_type=MESH,
        )

    def col_copy(k, dy, dc):
        there, core, device = at_y(dy, dc)
        return pltpu.make_async_remote_copy(
            src_ref=g_ref.at[:, pl.ds(pl.multiple_of((2 * (k % 4) + core) * width + k // 4 * part, part), part)],
            dst_ref=cols.at[me, k],
            send_sem=col_s.at[k, there * 2 + core],
            recv_sem=col_r.at[k, me],
            device_id=device,
            device_id_type=MESH,
        )

    def col_wait(k, slot):
        pltpu.make_async_remote_copy(
            src_ref=cols.at[slot, k],
            dst_ref=cols.at[slot, k],
            send_sem=col_s.at[k, slot],
            recv_sem=col_r.at[k, slot],
            device_id=at_y(0, 1)[2],
            device_id_type=MESH,
        ).wait_recv()

    def col_pass(k, core):
        step = 1 - 2 * core
        slot = ((y + 4 - step) % 4) * 2 + core
        return pltpu.make_async_remote_copy(
            src_ref=cols.at[slot, k],
            dst_ref=cols.at[slot, k],
            send_sem=col_s.at[k, ((y + 2) % 4) * 2 + core],
            recv_sem=col_r.at[k, slot],
            device_id=at_y(step + 4, 0)[2],
            device_id_type=MESH,
        )

    def w_copy(dx, owner):
        there, device = at_x(dx)
        slot = there if owner else x
        return pltpu.make_async_remote_copy(
            src_ref=w_ref.at[:, there],
            dst_ref=wparts.at[slot],
            send_sem=w_s.at[there],
            recv_sem=w_r.at[slot],
            device_id=device,
            device_id_type=MESH,
        )

    def send(u):
        for dy, dc in ((1, 0), (3, 0), (1, 1), (3, 1), (0, 1)):
            col_copy(unit_of(u), dy, dc).start()

    def forward(u):
        for core in (0, 1):
            slot = ((y + 3 + 2 * core) % 4) * 2 + core
            col_wait(unit_of(u), slot)
            col_pass(unit_of(u), core).start()

    for dy, dc in ((1, 0), (3, 0), (2, 0), (0, 1)):
        row_copy(dy, dc, False).start()
    send(0)
    send(1)
    for dx in (1, 2, 3):
        w_copy(dx, False).start()

    rows[me] = xt_ref[pl.ds(y * 2 * height, 2 * height), :]
    for k in range(4 * ROUNDS):
        start = pl.multiple_of((2 * (k % 4) + c) * width + k // 4 * part, part)
        cols[me, k] = g_ref[:, pl.ds(start, part)]
    wparts[x] = w_ref[:, x]

    for dy in (1, 3, 2):
        row_copy(dy, 0, True).wait_recv()
        row_pass(dy, False).start()
    forward(0)
    send(2)
    row_copy(0, 1, True).wait_recv()
    for dy in (1, 3, 2):
        row_pass(dy, True).wait_recv()

    def arrived(u):
        k = unit_of(u)
        for slot in (((y + 3) % 4) * 2 + 1, ((y + 1) % 4) * 2, y * 2 + 1 - c, ((y + 2) % 4) * 2, ((y + 2) % 4) * 2 + 1):
            col_wait(k, slot)

    scale = 1.0 / (seq * 64)
    main = jnp.where(low, 0, 1)
    place = jnp.where(low, z, 7 - z)

    def flip(d):
        return jnp.where(low, d, 7 - d)

    def coded_copy(way, d, s):
        span = pl.ds(s * piece, piece)
        return pltpu.make_async_remote_copy(
            src_ref=coded.at[way, d, span],
            dst_ref=coded.at[way, d, span],
            send_sem=coded_s.at[way, d, s],
            recv_sem=coded_r.at[way, d, s],
            device_id=at_z(1 - 2 * way),
            device_id_type=MESH,
        )

    def piece_of(s):
        return pl.ds(pl.multiple_of(s * piece, piece), piece)

    def first_step(r, away):
        d = r * 8 + flip(away)

        @pl.loop(0, SUBS)
        def _(s):
            coded[main, d, piece_of(s)] = encode(fisher[d, piece_of(s)] * scale + OFFSET)
            coded_copy(main, d, s).start()

    def step(way, r, away):
        d = r * 8 + flip(away)

        @pl.loop(0, SUBS)
        def _(s):
            coded_copy(way, d, s).wait_recv()
            own = fisher[d, piece_of(s)] * scale
            coded[way, d, piece_of(s)] = encode(decode(coded[way, d, piece_of(s)]) + own)
            coded_copy(way, d, s).start()

    def block(u, away, early):
        d = u // 4 * 8 + flip(away)
        k = unit_of(u)
        base = flip(away) // 4 * height

        @pl.loop(0, SUBS)
        def _(s):
            summed = None
            for slot in range(8):
                left = rows[slot, pl.ds(pl.multiple_of(base + s * piece, piece), piece), :]
                gradient = jnp.dot(left, cols[slot, k], preferred_element_type=jnp.float32)
                square = gradient * gradient
                summed = square if summed is None else summed + square
            fisher[d, piece_of(s)] = summed
            if early:
                @pl.when(place == 0)
                def _():
                    coded[main, d, piece_of(s)] = encode(summed * scale + OFFSET)
                    coded_copy(main, d, s).start()

    def steps(where, r, *aways):
        @pl.when(place == where)
        def _():
            for away in aways:
                if where == 0:
                    first_step(r, away)
                elif away < 0:
                    step(1 - main, r, -away % 8)
                else:
                    step(main, r, away)

    forward(1)
    send(3)
    arrived(0)
    block(0, 7, True)
    block(0, 3, True)
    forward(2)
    send(4)
    arrived(1)
    block(1, 6, True)
    block(1, 2, False)
    forward(3)
    send(5)
    steps(1, 0, 7)
    arrived(2)
    block(2, 5, True)
    block(2, 1, False)
    forward(4)
    send(6)
    steps(1, 0, 3, 6)
    steps(2, 0, 7)
    arrived(3)
    block(3, 4, True)
    block(3, 0, False)
    steps(0, 0, 2, 1)
    forward(5)
    send(7)
    steps(1, 0, 5)
    steps(2, 0, 3, 6)
    steps(3, 0, 7)
    arrived(4)
    block(4, 7, True)
    block(4, 3, False)
    forward(6)
    steps(1, 0, 4)
    steps(2, 0, 5)
    steps(3, 0, -8, 6)
    arrived(5)
    block(5, 6, True)
    block(5, 2, False)
    forward(7)
    steps(1, 0, 2)
    steps(2, 0, 4, -8)
    steps(3, 0, 5, -1)
    arrived(6)
    block(6, 5, True)
    block(6, 1, False)
    arrived(7)
    block(7, 4, True)
    block(7, 0, False)
    steps(0, 1, 3, 2, 1)
    steps(1, 0, -8)
    steps(1, 1, 7, 6, 5)
    steps(2, 0, -1)
    steps(2, 1, 7)
    steps(3, 0, 4, -2)

    def part_copy(r, s, dx, owner):
        there, device = at_x(dx)
        slot = there if owner else x
        return pltpu.make_async_remote_copy(
            src_ref=total.at[r, s, there],
            dst_ref=parts.at[r, s, slot],
            send_sem=part_s.at[r, s, there],
            recv_sem=part_r.at[r, s, slot],
            device_id=device,
            device_id_type=MESH,
        )

    def far_copies(r, s):
        return [
            pltpu.make_async_remote_copy(
                src_ref=here.at[r, s],
                dst_ref=there.at[r, s],
                send_sem=far_s.at[kind, r, s],
                recv_sem=far_r.at[kind, r, s],
                device_id=at_z(8),
                device_id_type=MESH,
            )
            for kind, (here, there) in enumerate(((tops, far_tops), (bottoms, far_bottoms)))
        ]

    def out_copy(r, s, dx, owner):
        there, device = at_x(dx)
        slot = there if owner else x
        return pltpu.make_async_remote_copy(
            src_ref=merged.at[r, s, slot],
            dst_ref=merged.at[r, s, slot],
            send_sem=out_s.at[r, s, there],
            recv_sem=out_r.at[r, s, slot],
            device_id=device,
            device_id_type=MESH,
        )

    def finish(r, s):
        base = s * piece
        own = r * 8 + z
        coded_copy(1 - main, own, s).wait_recv()

        @pl.when(place == 0)
        def _():
            for q in range(4):
                span = slice(base + q * band, base + (q + 1) * band)
                total[r, s, q] = fisher[own, span] * scale + OFFSET + decode(coded[1 - main, own, span])

        @pl.when(place > 0)
        def _():
            coded_copy(main, own, s).wait_recv()
            for q in range(4):
                span = slice(base + q * band, base + (q + 1) * band)
                total[r, s, q] = (
                    fisher[own, span] * scale + decode(coded[main, own, span]) + decode(coded[1 - main, own, span])
                )

        for dx in (1, 2, 3):
            part_copy(r, s, dx, False).start()
        parts[r, s, x] = total[r, s, x]

    def weigh(r, s):
        for dx in (1, 2, 3):
            part_copy(r, s, dx, True).wait_recv()
        damped = [parts[r, s, m] for m in range(4)]
        product = [damped[m] * wparts[m, s, :, r * part:(r + 1) * part] for m in range(4)]
        tops[r, s] = (product[0] + product[1]) + (product[2] + product[3])
        bottoms[r, s] = encode(((damped[0] + damped[1]) + (damped[2] + damped[3])) * 0.25)
        for copy in far_copies(r, s):
            copy.start()

    def merge(r, s):
        for copy in far_copies(r, s):
            copy.wait_recv()
        bottom = decode(bottoms[r, s]) + decode(far_bottoms[r, s])
        merged[r, s, x] = (tops[r, s] + far_tops[r, s]) * 0.25 / bottom
        for dx in (1, 2, 3):
            out_copy(r, s, dx, False).start()

    for s in range(SUBS):
        finish(0, s)
    steps(1, 1, 4)
    steps(2, 1, 6)
    for dx in (1, 2, 3):
        w_copy(dx, True).wait_recv()
    for s in range(SUBS):
        weigh(0, s)
    steps(1, 1, 3, 2, -8)
    steps(2, 1, 5, 4, 3, -8, -1)
    steps(3, 1, 7, 6, -8, 5, -1, 4, -2)
    for s in range(SUBS):
        finish(1, s)
    for s in range(SUBS):
        weigh(1, s)
    for r in range(ROUNDS):
        for s in range(SUBS):
            merge(r, s)
    for r in range(ROUNDS):
        for s in range(SUBS):
            for dx in (1, 2, 3):
                out_copy(r, s, dx, True).wait_recv()
        out_ref[:, :, :, r * part:(r + 1) * part] = merged[r]

    for dy, dc in ((1, 0), (3, 0), (2, 0), (0, 1)):
        row_copy(dy, dc, False).wait_send()
    for dy in (1, 3, 2):
        row_pass(dy, False).wait_send()

    @pl.loop(0, 4 * ROUNDS)
    def _(k):
        for dy, dc in ((1, 0), (3, 0), (1, 1), (3, 1), (0, 1)):
            col_copy(k, dy, dc).wait_send()
        for core in (0, 1):
            col_pass(k, core).wait_send()

    for dx in (1, 2, 3):
        w_copy(dx, False).wait_send()
        for r in range(ROUNDS):
            for s in range(SUBS):
                part_copy(r, s, dx, False).wait_send()
                out_copy(r, s, dx, False).wait_send()
    for r in range(ROUNDS):
        for s in range(SUBS):
            for copy in far_copies(r, s):
                copy.wait_send()

    @pl.loop(0, 8)
    def _(away):
        @pl.when(away != place)
        def _():
            for r in range(ROUNDS):
                for s in range(SUBS):
                    coded_copy(jnp.where(away > place, main, 1 - main), r * 8 + flip(away), s).wait_send()


def shards(inputs, cotangent, token_ids, weights):
    seq, feature = inputs.shape[2:]
    query = cotangent.shape[3]
    height, width = weights.shape[2:]
    band = height // SUBS // 4
    part = width // ROUNDS
    blocks = weights[0, 0].reshape(SUBS, 4, band, width)
    vmem = pl.BlockSpec(memory_space=pltpu.VMEM)
    dma = pltpu.SemaphoreType.DMA
    merged = pl.pallas_call(
        kernel,
        out_shape=jax.ShapeDtypeStruct((SUBS, 4, band, width), jnp.float32),
        in_specs=[pl.BlockSpec(memory_space=pl.ANY)] * 3 + [vmem],
        out_specs=vmem,
        scratch_shapes=[
            pltpu.VMEM((seq, feature), jnp.bfloat16),
            pltpu.VMEM((feature, seq), jnp.bfloat16),
            pltpu.VMEM((seq, query), jnp.bfloat16),
            pltpu.VMEM((SUBS, 4, band, width), jnp.float32),
            pltpu.VMEM((8, 2 * height, seq), jnp.bfloat16),
            pltpu.VMEM((8, 4 * ROUNDS, seq, part), jnp.bfloat16),
            pltpu.VMEM((8 * ROUNDS, height, part), jnp.float32),
            pltpu.VMEM((2, 8 * ROUNDS, height, part), jnp.bfloat16),
            pltpu.VMEM((ROUNDS, SUBS, 4, band, part), jnp.float32),
            pltpu.VMEM((ROUNDS, SUBS, 4, band, part), jnp.float32),
            pltpu.VMEM((4, SUBS, band, width), jnp.float32),
            pltpu.VMEM((ROUNDS, SUBS, band, part), jnp.float32),
            pltpu.VMEM((ROUNDS, SUBS, band, part), jnp.bfloat16),
            pltpu.VMEM((ROUNDS, SUBS, band, part), jnp.float32),
            pltpu.VMEM((ROUNDS, SUBS, band, part), jnp.bfloat16),
            pltpu.VMEM((ROUNDS, SUBS, 4, band, part), jnp.float32),
            dma((3,)),
            dma((8,)), dma((8,)), dma((4 * ROUNDS, 8)), dma((4 * ROUNDS, 8)),
            dma((2, 8 * ROUNDS, SUBS)), dma((2, 8 * ROUNDS, SUBS)),
            dma((4,)), dma((4,)), dma((ROUNDS, SUBS, 4)), dma((ROUNDS, SUBS, 4)),
            dma((2, ROUNDS, SUBS)), dma((2, ROUNDS, SUBS)), dma((ROUNDS, SUBS, 4)), dma((ROUNDS, SUBS, 4)),
        ],
        compiler_params=pltpu.CompilerParams(collective_id=0, has_side_effects=True),
    )(inputs[0, 0], cotangent[0, 0], blocks, token_ids[0])
    return merged.reshape(1, height, width)


def solution(mesh):
    in_specs = (
        P("mp", "tok", None, None),
        P("mp", "tok", None, None),
        P("mp", "tok", None),
        P("mp", "tok", None, None),
    )
    out_specs = P("tok", None, None)
    return jax.shard_map(shards, mesh=mesh, in_specs=in_specs, out_specs=out_specs, check_vma=False)
```

```python
import jax
import jax.numpy as jnp
from jax import lax
from jax.experimental import pallas as pl
from jax.experimental.pallas import tpu as pltpu
from jax.sharding import PartitionSpec as P

FIRST_TEXT = 37984
DAMPING = 0.1
WIDTHS = (256, 256)
ROUNDS = len(WIDTHS)
STARTS = tuple(sum(WIDTHS[:r]) for r in range(ROUNDS))
SUBS = 4
HALVES = 2
MESH = pl.DeviceIdType.MESH
Y_PEERS = ((1, 0), (3, 0), (1, 1), (3, 1), (2, 0), (2, 1), (0, 1))
OFFSET = DAMPING / 2
MIDDLE = 90.5
LOW_UNIT = 2.0
HIGH_UNIT = 4096.0


def encode(values):
    small = values < MIDDLE
    ratio = values * jnp.where(small, 1.0 / LOW_UNIT, 1.0 / HIGH_UNIT)
    square = ratio * ratio
    fourth = square * square
    eighth = fourth * fourth
    power = (eighth * eighth) * (fourth * square)
    return jnp.where(small, power, -power).astype(jnp.bfloat16)


def decode(code):
    power = code.astype(jnp.float32)
    ratio = jnp.exp2(jnp.log2(jnp.abs(power)) * (1.0 / 22))
    return ratio * jnp.where(power > 0, LOW_UNIT, HIGH_UNIT)


def kernel(
    x_hbm, g_hbm, w_hbm, ids_ref, out_ref,
    x_ref, xt_ref, g_ref, w_ref, rows, cols, fisher, coded, total, parts, wparts,
    tops, bottoms, far_tops, far_bottoms, merged, load_s,
    row_s, row_r, col_s, col_r, coded_s, coded_r,
    w_s, w_r, part_s, part_r, far_s, far_r, out_s, out_r,
):
    loads = (
        pltpu.make_async_copy(x_hbm, x_ref, load_s.at[0]),
        pltpu.make_async_copy(g_hbm, g_ref, load_s.at[1]),
        pltpu.make_async_copy(w_hbm, w_ref, load_s.at[2]),
    )
    for load in (loads[1], loads[0], loads[2]):
        load.start()
    mp = lax.axis_index("mp")
    tok = lax.axis_index("tok")
    x, zh = mp // 2, mp % 2
    y, z, c = tok // 16, (tok // 2) % 8, tok % 2
    me = y * 2 + c
    seq = g_ref.shape[0]
    width = w_ref.shape[3]
    height = w_ref.shape[0] * w_ref.shape[1] * w_ref.shape[2]
    piece = height // SUBS
    band = height // HALVES // 4

    def at_y(dy, dc):
        there = (y + dy) % 4
        core = 1 - c if dc else c
        return there, core, (mp, (there * 8 + z) * 2 + core)

    def at_x(dx):
        there = (x + dx) % 4
        return there, (there * 2 + zh, tok)

    def at_z(dz):
        deep = zh * 8 + z + dz + 16
        return (x * 2 + (deep // 8) % 2, (y * 8 + deep % 8) * 2 + c)

    barrier = pltpu.get_barrier_semaphore()
    for dy, dc in Y_PEERS:
        pl.semaphore_signal(barrier, 1, device_id=at_y(dy, dc)[2], device_id_type=MESH)
    for dx in (1, 2, 3):
        pl.semaphore_signal(barrier, 1, device_id=at_x(dx)[1], device_id_type=MESH)
    for dz in (1, -1, 8):
        pl.semaphore_signal(barrier, 1, device_id=at_z(dz), device_id_type=MESH)
    pl.semaphore_wait(barrier, len(Y_PEERS) + 6)

    loads[1].wait()

    low = z < 4

    def unit_of(u):
        return u // 4, jnp.where(low, 3 - u % 4, u % 4)

    def columns(r, k, core):
        return pl.ds(pl.multiple_of((2 * k + core) * width + STARTS[r], 128), WIDTHS[r])

    def row_copy(dy, dc, owner):
        there, core, device = at_y(dy, dc)
        slot = there * 2 + core if owner else me
        return pltpu.make_async_remote_copy(
            src_ref=xt_ref.at[pl.ds(there * 2 * height, 2 * height)],
            dst_ref=rows.at[slot],
            send_sem=row_s.at[there * 2 + core],
            recv_sem=row_r.at[slot],
            device_id=device,
            device_id_type=MESH,
        )

    def row_pass(dy, owner):
        there = (y + dy) % 4
        slot = there * 2 + (1 - c if owner else c)
        return pltpu.make_async_remote_copy(
            src_ref=rows.at[slot],
            dst_ref=rows.at[slot],
            send_sem=row_s.at[there * 2 + 1 - c],
            recv_sem=row_r.at[slot],
            device_id=at_y(0, 1)[2],
            device_id_type=MESH,
        )

    def col_copy(r, k, dy, dc):
        there, core, device = at_y(dy, dc)
        return pltpu.make_async_remote_copy(
            src_ref=g_ref.at[:, columns(r, k, core)],
            dst_ref=cols[r].at[me, k],
            send_sem=col_s.at[r, k, there * 2 + core],
            recv_sem=col_r.at[r, k, me],
            device_id=device,
            device_id_type=MESH,
        )

    def col_wait(r, k, slot):
        pltpu.make_async_remote_copy(
            src_ref=cols[r].at[slot, k],
            dst_ref=cols[r].at[slot, k],
            send_sem=col_s.at[r, k, slot],
            recv_sem=col_r.at[r, k, slot],
            device_id=at_y(0, 1)[2],
            device_id_type=MESH,
        ).wait_recv()

    def col_pass(r, k, core):
        step = 1 - 2 * core
        slot = ((y + 4 - step) % 4) * 2 + core
        return pltpu.make_async_remote_copy(
            src_ref=cols[r].at[slot, k],
            dst_ref=cols[r].at[slot, k],
            send_sem=col_s.at[r, k, ((y + 2) % 4) * 2 + core],
            recv_sem=col_r.at[r, k, slot],
            device_id=at_y(step + 4, 0)[2],
            device_id_type=MESH,
        )

    def w_copy(dx, owner):
        there, device = at_x(dx)
        slot = there if owner else x
        return pltpu.make_async_remote_copy(
            src_ref=w_ref.at[:, there],
            dst_ref=wparts.at[slot],
            send_sem=w_s.at[there],
            recv_sem=w_r.at[slot],
            device_id=device,
            device_id_type=MESH,
        )

    def send(u):
        for dy, dc in ((1, 0), (3, 0), (1, 1), (3, 1), (0, 1)):
            col_copy(*unit_of(u), dy, dc).start()

    def forward(u):
        for core in (0, 1):
            slot = ((y + 3 + 2 * core) % 4) * 2 + core
            col_wait(*unit_of(u), slot)
            col_pass(*unit_of(u), core).start()

    send(0)

    loads[0].wait()
    kept = ids_ref[...] >= FIRST_TEXT
    for r in range(8):
        some = x_ref[:, r * height:(r + 1) * height].astype(jnp.float32).T
        xt_ref[r * height:(r + 1) * height, :] = jnp.where(kept, some, 0.0).astype(jnp.bfloat16)

    for dy, dc in ((1, 0), (3, 0), (2, 0), (0, 1)):
        row_copy(dy, dc, False).start()
    send(1)
    loads[2].wait()
    for dx in (1, 2, 3):
        w_copy(dx, False).start()

    rows[me] = xt_ref[pl.ds(y * 2 * height, 2 * height), :]
    for r in range(ROUNDS):
        for k in range(4):
            cols[r][me, k] = g_ref[:, columns(r, k, c)]
    wparts[x] = w_ref[:, x]

    forward(0)
    for dy in (1, 3, 2):
        row_copy(dy, 0, True).wait_recv()
        row_pass(dy, False).start()
    send(2)
    row_copy(0, 1, True).wait_recv()
    for dy in (1, 3, 2):
        row_pass(dy, True).wait_recv()

    def arrived(u):
        r, k = unit_of(u)
        for slot in (((y + 3) % 4) * 2 + 1, ((y + 1) % 4) * 2, y * 2 + 1 - c, ((y + 2) % 4) * 2, ((y + 2) % 4) * 2 + 1):
            col_wait(r, k, slot)

    scale = 1.0 / (seq * 64)
    main = jnp.where(low, 0, 1)
    place = jnp.where(low, z, 7 - z)

    def flip(d):
        return jnp.where(low, d, 7 - d)

    def coded_copy(way, r, d, s):
        span = pl.ds(s * piece, piece)
        return pltpu.make_async_remote_copy(
            src_ref=coded[r].at[way, d, span],
            dst_ref=coded[r].at[way, d, span],
            send_sem=coded_s.at[way, r, d],
            recv_sem=coded_r.at[way, r, d, s],
            device_id=at_z(1 - 2 * way),
            device_id_type=MESH,
        )

    def coded_sent(way, r, d):
        pltpu.make_async_remote_copy(
            src_ref=coded[r].at[way, d],
            dst_ref=coded[r].at[way, d],
            send_sem=coded_s.at[way, r, d],
            recv_sem=coded_r.at[way, r, d, 0],
            device_id=at_z(1 - 2 * way),
            device_id_type=MESH,
        ).wait_send()

    def piece_of(s):
        return pl.ds(pl.multiple_of(s * piece, piece), piece)

    def first_step(r, away):
        d = flip(away)

        @pl.loop(0, SUBS)
        def _(s):
            coded[r][main, d, piece_of(s)] = encode(fisher[r][d, piece_of(s)] * scale + OFFSET)
            coded_copy(main, r, d, s).start()

    def step(way, r, away):
        d = flip(away)

        @pl.loop(0, SUBS)
        def _(s):
            coded_copy(way, r, d, s).wait_recv()
            own = fisher[r][d, piece_of(s)] * scale
            coded[r][way, d, piece_of(s)] = encode(decode(coded[r][way, d, piece_of(s)]) + own)
            coded_copy(way, r, d, s).start()

    def block(u, away, early):
        r, k = unit_of(u)
        d = flip(away)
        base = d // 4 * height

        @pl.loop(0, SUBS)
        def _(s):
            summed = None
            for slot in range(8):
                left = rows[slot, pl.ds(pl.multiple_of(base + s * piece, piece), piece), :]
                gradient = jnp.dot(left, cols[r][slot, k], preferred_element_type=jnp.float32)
                square = gradient * gradient
                summed = square if summed is None else summed + square
            fisher[r][d, piece_of(s)] = summed
            if early:
                @pl.when(place == 0)
                def _():
                    coded[r][main, d, piece_of(s)] = encode(summed * scale + OFFSET)
                    coded_copy(main, r, d, s).start()

    def steps(where, r, *aways):
        @pl.when(place == where)
        def _():
            for away in aways:
                if where == 0:
                    first_step(r, away)
                elif away < 0:
                    step(1 - main, r, -away % 8)
                else:
                    step(main, r, away)

    forward(1)
    send(3)
    arrived(0)
    block(0, 7, True)
    block(0, 3, True)
    forward(2)
    send(4)
    arrived(1)
    block(1, 6, True)
    block(1, 2, False)
    forward(3)
    send(5)
    steps(1, 0, 7)
    arrived(2)
    block(2, 5, True)
    block(2, 1, False)
    forward(4)
    send(6)
    steps(1, 0, 3, 6)
    steps(2, 0, 7)
    arrived(3)
    block(3, 4, True)
    block(3, 0, False)
    steps(0, 0, 2, 1)
    forward(5)
    send(7)
    steps(1, 0, 5)
    steps(2, 0, 3, 6)
    steps(3, 0, 7)
    arrived(4)
    block(4, 7, True)
    block(4, 3, False)
    forward(6)
    steps(1, 0, 4)
    steps(2, 0, 5)
    steps(3, 0, -8, 6)
    arrived(5)
    block(5, 6, True)
    block(5, 2, False)
    forward(7)
    steps(1, 0, 2)
    steps(2, 0, 4, -8)
    steps(3, 0, 5, -1)
    arrived(6)
    block(6, 5, True)
    block(6, 1, False)
    arrived(7)
    block(7, 4, True)
    block(7, 0, False)
    steps(0, 1, 3, 2, 1)
    steps(1, 0, -8)
    steps(1, 1, 7, 6, 5)
    steps(2, 0, -1)
    steps(2, 1, 7)
    steps(3, 0, 4, -2)

    def part_copy(r, s, dx, owner):
        there, device = at_x(dx)
        slot = there if owner else x
        return pltpu.make_async_remote_copy(
            src_ref=total[r].at[s, there],
            dst_ref=parts[r].at[s, slot],
            send_sem=part_s.at[r, s, there],
            recv_sem=part_r.at[r, s, slot],
            device_id=device,
            device_id_type=MESH,
        )

    def far_copies(r, s):
        return [
            pltpu.make_async_remote_copy(
                src_ref=here[r].at[s],
                dst_ref=there[r].at[s],
                send_sem=far_s.at[kind, r, s],
                recv_sem=far_r.at[kind, r, s],
                device_id=at_z(8),
                device_id_type=MESH,
            )
            for kind, (here, there) in enumerate(((tops, far_tops), (bottoms, far_bottoms)))
        ]

    def out_copy(r, s, dx, owner):
        there, device = at_x(dx)
        slot = there if owner else x
        return pltpu.make_async_remote_copy(
            src_ref=merged[r].at[s, slot],
            dst_ref=merged[r].at[s, slot],
            send_sem=out_s.at[r, s, there],
            recv_sem=out_r.at[r, s, slot],
            device_id=device,
            device_id_type=MESH,
        )

    def finish(r, s):
        base = s * 4 * band
        inner = range(s * SUBS // HALVES, (s + 1) * SUBS // HALVES)
        for one in inner:
            coded_copy(1 - main, r, z, one).wait_recv()

        @pl.when(place == 0)
        def _():
            for q in range(4):
                span = slice(base + q * band, base + (q + 1) * band)
                total[r][s, q] = fisher[r][z, span] * scale + OFFSET + decode(coded[r][1 - main, z, span])

        @pl.when(place > 0)
        def _():
            for one in inner:
                coded_copy(main, r, z, one).wait_recv()
            for q in range(4):
                span = slice(base + q * band, base + (q + 1) * band)
                total[r][s, q] = (
                    fisher[r][z, span] * scale + decode(coded[r][main, z, span]) + decode(coded[r][1 - main, z, span])
                )

        for dx in (1, 2, 3):
            part_copy(r, s, dx, False).start()
        parts[r][s, x] = total[r][s, x]

    def weigh(r, s):
        for dx in (1, 2, 3):
            part_copy(r, s, dx, True).wait_recv()
        damped = [parts[r][s, m] for m in range(4)]
        product = [damped[m] * wparts[m, s, :, STARTS[r]:STARTS[r] + WIDTHS[r]] for m in range(4)]
        tops[r][s] = (product[0] + product[1]) + (product[2] + product[3])
        bottoms[r][s] = encode(((damped[0] + damped[1]) + (damped[2] + damped[3])) * 0.25)
        for copy in far_copies(r, s):
            copy.start()

    def merge(r, s):
        for copy in far_copies(r, s):
            copy.wait_recv()
        bottom = decode(bottoms[r][s]) + decode(far_bottoms[r][s])
        merged[r][s, x] = (tops[r][s] + far_tops[r][s]) * 0.25 / bottom
        for dx in (1, 2, 3):
            out_copy(r, s, dx, False).start()

    for s in range(HALVES):
        finish(0, s)
    steps(1, 1, 4)
    steps(2, 1, 6)
    for dx in (1, 2, 3):
        w_copy(dx, True).wait_recv()
    for s in range(HALVES):
        weigh(0, s)
    steps(1, 1, 3, 2, -8)
    steps(2, 1, 5, 4, 3, -8, -1)
    steps(3, 1, 7, 6, -8, 5, -1, 4, -2)
    for s in range(HALVES):
        finish(1, s)
    for s in range(HALVES):
        weigh(1, s)
    for r in range(ROUNDS):
        for s in range(HALVES):
            merge(r, s)
    for r in range(ROUNDS):
        for s in range(HALVES):
            for dx in (1, 2, 3):
                out_copy(r, s, dx, True).wait_recv()
        out_ref[:, :, :, STARTS[r]:STARTS[r] + WIDTHS[r]] = merged[r][...]

    for dy, dc in ((1, 0), (3, 0), (2, 0), (0, 1)):
        row_copy(dy, dc, False).wait_send()
    for dy in (1, 3, 2):
        row_pass(dy, False).wait_send()

    @pl.loop(0, 4)
    def _(k):
        for r in range(ROUNDS):
            for dy, dc in ((1, 0), (3, 0), (1, 1), (3, 1), (0, 1)):
                col_copy(r, k, dy, dc).wait_send()
            for core in (0, 1):
                col_pass(r, k, core).wait_send()

    for dx in (1, 2, 3):
        w_copy(dx, False).wait_send()
        for r in range(ROUNDS):
            for s in range(HALVES):
                part_copy(r, s, dx, False).wait_send()
                out_copy(r, s, dx, False).wait_send()
    for r in range(ROUNDS):
        for s in range(HALVES):
            for copy in far_copies(r, s):
                copy.wait_send()

    @pl.loop(0, 8)
    def _(away):
        @pl.when(away != place)
        def _():
            for r in range(ROUNDS):
                coded_sent(jnp.where(away > place, main, 1 - main), r, flip(away))


def shards(inputs, cotangent, token_ids, weights):
    seq, feature = inputs.shape[2:]
    query = cotangent.shape[3]
    height, width = weights.shape[2:]
    band = height // HALVES // 4
    blocks = weights[0, 0].reshape(HALVES, 4, band, width)
    vmem = pl.BlockSpec(memory_space=pltpu.VMEM)
    dma = pltpu.SemaphoreType.DMA
    merged = pl.pallas_call(
        kernel,
        out_shape=jax.ShapeDtypeStruct((HALVES, 4, band, width), jnp.float32),
        in_specs=[pl.BlockSpec(memory_space=pl.ANY)] * 3 + [vmem],
        out_specs=vmem,
        scratch_shapes=[
            pltpu.VMEM((seq, feature), jnp.bfloat16),
            pltpu.VMEM((feature, seq), jnp.bfloat16),
            pltpu.VMEM((seq, query), jnp.bfloat16),
            pltpu.VMEM((HALVES, 4, band, width), jnp.float32),
            pltpu.VMEM((8, 2 * height, seq), jnp.bfloat16),
            [pltpu.VMEM((8, 4, seq, part), jnp.bfloat16) for part in WIDTHS],
            [pltpu.VMEM((8, height, part), jnp.float32) for part in WIDTHS],
            [pltpu.VMEM((2, 8, height, part), jnp.bfloat16) for part in WIDTHS],
            [pltpu.VMEM((HALVES, 4, band, part), jnp.float32) for part in WIDTHS],
            [pltpu.VMEM((HALVES, 4, band, part), jnp.float32) for part in WIDTHS],
            pltpu.VMEM((4, HALVES, band, width), jnp.float32),
            [pltpu.VMEM((HALVES, band, part), jnp.float32) for part in WIDTHS],
            [pltpu.VMEM((HALVES, band, part), jnp.bfloat16) for part in WIDTHS],
            [pltpu.VMEM((HALVES, band, part), jnp.float32) for part in WIDTHS],
            [pltpu.VMEM((HALVES, band, part), jnp.bfloat16) for part in WIDTHS],
            [pltpu.VMEM((HALVES, 4, band, part), jnp.float32) for part in WIDTHS],
            dma((3,)),
            dma((8,)), dma((8,)), dma((ROUNDS, 4, 8)), dma((ROUNDS, 4, 8)),
            dma((2, ROUNDS, 8)), dma((2, ROUNDS, 8, SUBS)),
            dma((4,)), dma((4,)), dma((ROUNDS, HALVES, 4)), dma((ROUNDS, HALVES, 4)),
            dma((2, ROUNDS, HALVES)), dma((2, ROUNDS, HALVES)), dma((ROUNDS, HALVES, 4)), dma((ROUNDS, HALVES, 4)),
        ],
        compiler_params=pltpu.CompilerParams(collective_id=0, has_side_effects=True),
    )(inputs[0, 0], cotangent[0, 0], blocks, token_ids[0])
    return merged.reshape(1, height, width)


def solution(mesh):
    in_specs = (
        P("mp", "tok", None, None),
        P("mp", "tok", None, None),
        P("mp", "tok", None),
        P("mp", "tok", None, None),
    )
    out_specs = P("tok", None, None)
    return jax.shard_map(shards, mesh=mesh, in_specs=in_specs, out_specs=out_specs, check_vma=False)
```

```python
import jax
import jax.numpy as jnp
from jax import lax
from jax.experimental import pallas as pl
from jax.experimental.pallas import tpu as pltpu
from jax.sharding import PartitionSpec as P

FIRST_TEXT = 37984
DAMPING = 0.1
WIDTHS = (256, 256)
ROUNDS = len(WIDTHS)
STARTS = tuple(sum(WIDTHS[:r]) for r in range(ROUNDS))
SUBS = 4
HALVES = 2
MESH = pl.DeviceIdType.MESH
Y_PEERS = ((1, 0), (3, 0), (1, 1), (3, 1), (2, 0), (2, 1), (0, 1))
OFFSET = DAMPING / 2
MIDDLE = 90.5
LOW_UNIT = 2.0
HIGH_UNIT = 4096.0


def encode(values):
    small = values < MIDDLE
    ratio = values * jnp.where(small, 1.0 / LOW_UNIT, 1.0 / HIGH_UNIT)
    square = ratio * ratio
    fourth = square * square
    eighth = fourth * fourth
    power = (eighth * eighth) * (fourth * square)
    return jnp.where(small, power, -power).astype(jnp.bfloat16)


def decode(code):
    power = code.astype(jnp.float32)
    ratio = jnp.exp2(jnp.log2(jnp.abs(power)) * (1.0 / 22))
    return ratio * jnp.where(power > 0, LOW_UNIT, HIGH_UNIT)


def kernel(
    x_hbm, g_hbm, w_hbm, ids_ref, out_ref,
    x_ref, xt_ref, g_ref, w_ref, rows, cols, fisher, coded, total, parts, wparts,
    tops, bottoms, far_tops, far_bottoms, merged, load_s,
    row_s, row_r, col_s, col_r, coded_s, coded_r,
    w_s, w_r, part_s, part_r, far_s, far_r, out_s, out_r,
):
    loads = (
        pltpu.make_async_copy(x_hbm, x_ref, load_s.at[0]),
        pltpu.make_async_copy(g_hbm, g_ref, load_s.at[1]),
        pltpu.make_async_copy(w_hbm, w_ref, load_s.at[2]),
    )
    for load in (loads[1], loads[0], loads[2]):
        load.start()
    mp = lax.axis_index("mp")
    tok = lax.axis_index("tok")
    x, zh = mp // 2, mp % 2
    y, z, c = tok // 16, (tok // 2) % 8, tok % 2
    me = y * 2 + c
    seq = g_ref.shape[0]
    width = w_ref.shape[3]
    height = w_ref.shape[0] * w_ref.shape[1] * w_ref.shape[2]
    piece = height // SUBS
    band = height // HALVES // 4

    def at_y(dy, dc):
        there = (y + dy) % 4
        core = 1 - c if dc else c
        return there, core, (mp, (there * 8 + z) * 2 + core)

    def at_x(dx):
        there = (x + dx) % 4
        return there, (there * 2 + zh, tok)

    def at_z(dz):
        deep = zh * 8 + z + dz + 16
        return (x * 2 + (deep // 8) % 2, (y * 8 + deep % 8) * 2 + c)

    barrier = pltpu.get_barrier_semaphore()
    for dy, dc in Y_PEERS:
        pl.semaphore_signal(barrier, 1, device_id=at_y(dy, dc)[2], device_id_type=MESH)
    for dx in (1, 2, 3):
        pl.semaphore_signal(barrier, 1, device_id=at_x(dx)[1], device_id_type=MESH)
    for dz in (1, -1, 8):
        pl.semaphore_signal(barrier, 1, device_id=at_z(dz), device_id_type=MESH)
    pl.semaphore_wait(barrier, len(Y_PEERS) + 6)

    loads[1].wait()

    low = z < 4

    def unit_of(u):
        return u // 4, jnp.where(low, 3 - u % 4, u % 4)

    def columns(r, k, core):
        return pl.ds(pl.multiple_of((2 * k + core) * width + STARTS[r], 128), WIDTHS[r])

    def row_copy(dy, dc, owner):
        there, core, device = at_y(dy, dc)
        slot = there * 2 + core if owner else me
        return pltpu.make_async_remote_copy(
            src_ref=xt_ref.at[pl.ds(there * 2 * height, 2 * height)],
            dst_ref=rows.at[slot],
            send_sem=row_s.at[there * 2 + core],
            recv_sem=row_r.at[slot],
            device_id=device,
            device_id_type=MESH,
        )

    def row_pass(dy, owner):
        there = (y + dy) % 4
        slot = there * 2 + (1 - c if owner else c)
        return pltpu.make_async_remote_copy(
            src_ref=rows.at[slot],
            dst_ref=rows.at[slot],
            send_sem=row_s.at[there * 2 + 1 - c],
            recv_sem=row_r.at[slot],
            device_id=at_y(0, 1)[2],
            device_id_type=MESH,
        )

    def col_copy(r, k, dy, dc):
        there, core, device = at_y(dy, dc)
        return pltpu.make_async_remote_copy(
            src_ref=g_ref.at[:, columns(r, k, core)],
            dst_ref=cols[r].at[me, k],
            send_sem=col_s.at[r, k, there * 2 + core],
            recv_sem=col_r.at[r, k, me],
            device_id=device,
            device_id_type=MESH,
        )

    def col_wait(r, k, slot):
        pltpu.make_async_remote_copy(
            src_ref=cols[r].at[slot, k],
            dst_ref=cols[r].at[slot, k],
            send_sem=col_s.at[r, k, slot],
            recv_sem=col_r.at[r, k, slot],
            device_id=at_y(0, 1)[2],
            device_id_type=MESH,
        ).wait_recv()

    def col_pass(r, k, core):
        step = 1 - 2 * core
        slot = ((y + 4 - step) % 4) * 2 + core
        return pltpu.make_async_remote_copy(
            src_ref=cols[r].at[slot, k],
            dst_ref=cols[r].at[slot, k],
            send_sem=col_s.at[r, k, ((y + 2) % 4) * 2 + core],
            recv_sem=col_r.at[r, k, slot],
            device_id=at_y(step + 4, 0)[2],
            device_id_type=MESH,
        )

    def w_copy(dx, owner):
        there, device = at_x(dx)
        slot = there if owner else x
        return pltpu.make_async_remote_copy(
            src_ref=w_ref.at[:, there],
            dst_ref=wparts.at[slot],
            send_sem=w_s.at[there],
            recv_sem=w_r.at[slot],
            device_id=device,
            device_id_type=MESH,
        )

    def send(u):
        for dy in (1 + 2 * c, 3 - 2 * c):
            for dc in (0, 1):
                col_copy(*unit_of(u), dy, dc).start()
        col_copy(*unit_of(u), 0, 1).start()

    def forward(u):
        for core in (0, 1):
            slot = ((y + 3 + 2 * core) % 4) * 2 + core
            col_wait(*unit_of(u), slot)
            col_pass(*unit_of(u), core).start()

    send(0)

    loads[0].wait()
    kept = ids_ref[...] >= FIRST_TEXT
    for r in range(8):
        some = x_ref[:, r * height:(r + 1) * height].astype(jnp.float32).T
        xt_ref[r * height:(r + 1) * height, :] = jnp.where(kept, some, 0.0).astype(jnp.bfloat16)

    for dy, dc in ((1, 0), (3, 0), (2, 0), (0, 1)):
        row_copy(dy, dc, False).start()
    send(1)
    loads[2].wait()
    for dx in (1, 2, 3):
        w_copy(dx, False).start()

    rows[me] = xt_ref[pl.ds(y * 2 * height, 2 * height), :]
    for r in range(ROUNDS):
        for k in range(4):
            cols[r][me, k] = g_ref[:, columns(r, k, c)]
    wparts[x] = w_ref[:, x]

    forward(0)
    for dy in (1, 3, 2):
        row_copy(dy, 0, True).wait_recv()
        row_pass(dy, False).start()
    send(2)
    row_copy(0, 1, True).wait_recv()
    for dy in (1, 3, 2):
        row_pass(dy, True).wait_recv()

    def arrived(u):
        r, k = unit_of(u)
        for slot in (((y + 3) % 4) * 2 + 1, ((y + 1) % 4) * 2, y * 2 + 1 - c, ((y + 2) % 4) * 2, ((y + 2) % 4) * 2 + 1):
            col_wait(r, k, slot)

    scale = 1.0 / (seq * 64)
    main = jnp.where(low, 0, 1)
    place = jnp.where(low, z, 7 - z)

    def flip(d):
        return jnp.where(low, d, 7 - d)

    def coded_copy(way, r, d, s):
        span = pl.ds(s * piece, piece)
        return pltpu.make_async_remote_copy(
            src_ref=coded[r].at[way, d, span],
            dst_ref=coded[r].at[way, d, span],
            send_sem=coded_s.at[way, r, d],
            recv_sem=coded_r.at[way, r, d, s],
            device_id=at_z(1 - 2 * way),
            device_id_type=MESH,
        )

    def coded_sent(way, r, d):
        pltpu.make_async_remote_copy(
            src_ref=coded[r].at[way, d],
            dst_ref=coded[r].at[way, d],
            send_sem=coded_s.at[way, r, d],
            recv_sem=coded_r.at[way, r, d, 0],
            device_id=at_z(1 - 2 * way),
            device_id_type=MESH,
        ).wait_send()

    def piece_of(s):
        return pl.ds(pl.multiple_of(s * piece, piece), piece)

    def first_step(r, away):
        d = flip(away)

        @pl.loop(0, SUBS)
        def _(s):
            coded[r][main, d, piece_of(s)] = encode(fisher[r][d, piece_of(s)] * scale + OFFSET)
            coded_copy(main, r, d, s).start()

    def step(way, r, away):
        d = flip(away)

        @pl.loop(0, SUBS)
        def _(s):
            coded_copy(way, r, d, s).wait_recv()
            own = fisher[r][d, piece_of(s)] * scale
            coded[r][way, d, piece_of(s)] = encode(decode(coded[r][way, d, piece_of(s)]) + own)
            coded_copy(way, r, d, s).start()

    def block(u, away, early):
        r, k = unit_of(u)
        d = flip(away)
        base = d // 4 * height

        @pl.loop(0, SUBS)
        def _(s):
            summed = None
            for slot in range(8):
                left = rows[slot, pl.ds(pl.multiple_of(base + s * piece, piece), piece), :]
                gradient = jnp.dot(left, cols[r][slot, k], preferred_element_type=jnp.float32)
                square = gradient * gradient
                summed = square if summed is None else summed + square
            fisher[r][d, piece_of(s)] = summed
            if early:
                @pl.when(place == 0)
                def _():
                    coded[r][main, d, piece_of(s)] = encode(summed * scale + OFFSET)
                    coded_copy(main, r, d, s).start()

    def steps(where, r, *aways):
        @pl.when(place == where)
        def _():
            for away in aways:
                if where == 0:
                    first_step(r, away)
                elif away < 0:
                    step(1 - main, r, -away % 8)
                else:
                    step(main, r, away)

    forward(1)
    send(3)
    arrived(0)
    block(0, 7, True)
    block(0, 3, True)
    forward(2)
    send(4)
    arrived(1)
    block(1, 6, True)
    block(1, 2, False)
    forward(3)
    send(5)
    steps(1, 0, 7)
    arrived(2)
    block(2, 5, True)
    block(2, 1, False)
    forward(4)
    send(6)
    steps(1, 0, 3, 6)
    steps(2, 0, 7)
    arrived(3)
    block(3, 4, True)
    block(3, 0, False)
    steps(0, 0, 2, 1)
    forward(5)
    send(7)
    steps(1, 0, 5)
    steps(2, 0, 3, 6)
    steps(3, 0, 7)
    arrived(4)
    block(4, 7, True)
    block(4, 3, False)
    forward(6)
    steps(1, 0, 4)
    steps(2, 0, 5)
    steps(3, 0, -8, 6)
    arrived(5)
    block(5, 6, True)
    block(5, 2, False)
    forward(7)
    steps(1, 0, 2)
    steps(2, 0, 4, -8)
    steps(3, 0, 5, -1)
    arrived(6)
    block(6, 5, True)
    block(6, 1, False)
    arrived(7)
    block(7, 4, True)
    block(7, 0, False)
    steps(0, 1, 3, 2, 1)
    steps(1, 0, -8)
    steps(1, 1, 7, 6, 5)
    steps(2, 0, -1)
    steps(2, 1, 7)
    steps(3, 0, 4, -2)

    def part_copy(r, s, dx, owner):
        there, device = at_x(dx)
        slot = there if owner else x
        return pltpu.make_async_remote_copy(
            src_ref=total[r].at[s, there],
            dst_ref=parts[r].at[s, slot],
            send_sem=part_s.at[r, s, there],
            recv_sem=part_r.at[r, s, slot],
            device_id=device,
            device_id_type=MESH,
        )

    def far_copies(r, s):
        return [
            pltpu.make_async_remote_copy(
                src_ref=here[r].at[s],
                dst_ref=there[r].at[s],
                send_sem=far_s.at[kind, r, s],
                recv_sem=far_r.at[kind, r, s],
                device_id=at_z(8),
                device_id_type=MESH,
            )
            for kind, (here, there) in enumerate(((tops, far_tops), (bottoms, far_bottoms)))
        ]

    def out_copy(r, s, dx, owner):
        there, device = at_x(dx)
        slot = there if owner else x
        return pltpu.make_async_remote_copy(
            src_ref=merged[r].at[s, slot],
            dst_ref=merged[r].at[s, slot],
            send_sem=out_s.at[r, s, there],
            recv_sem=out_r.at[r, s, slot],
            device_id=device,
            device_id_type=MESH,
        )

    def finish(r, s):
        base = s * 4 * band
        inner = range(s * SUBS // HALVES, (s + 1) * SUBS // HALVES)
        for one in inner:
            coded_copy(1 - main, r, z, one).wait_recv()

        @pl.when(place == 0)
        def _():
            for q in range(4):
                span = slice(base + q * band, base + (q + 1) * band)
                total[r][s, q] = fisher[r][z, span] * scale + OFFSET + decode(coded[r][1 - main, z, span])

        @pl.when(place > 0)
        def _():
            for one in inner:
                coded_copy(main, r, z, one).wait_recv()
            for q in range(4):
                span = slice(base + q * band, base + (q + 1) * band)
                total[r][s, q] = (
                    fisher[r][z, span] * scale + decode(coded[r][main, z, span]) + decode(coded[r][1 - main, z, span])
                )

        for dx in (1, 2, 3):
            part_copy(r, s, dx, False).start()
        parts[r][s, x] = total[r][s, x]

    def weigh(r, s):
        for dx in (1, 2, 3):
            part_copy(r, s, dx, True).wait_recv()
        damped = [parts[r][s, m] for m in range(4)]
        product = [damped[m] * wparts[m, s, :, STARTS[r]:STARTS[r] + WIDTHS[r]] for m in range(4)]
        tops[r][s] = (product[0] + product[1]) + (product[2] + product[3])
        bottoms[r][s] = encode(((damped[0] + damped[1]) + (damped[2] + damped[3])) * 0.25)
        for copy in far_copies(r, s):
            copy.start()

    def merge(r, s):
        for copy in far_copies(r, s):
            copy.wait_recv()
        bottom = decode(bottoms[r][s]) + decode(far_bottoms[r][s])
        merged[r][s, x] = (tops[r][s] + far_tops[r][s]) * 0.25 / bottom
        for dx in (1, 2, 3):
            out_copy(r, s, dx, False).start()

    for s in range(HALVES):
        finish(0, s)
    steps(1, 1, 4)
    steps(2, 1, 6)
    for dx in (1, 2, 3):
        w_copy(dx, True).wait_recv()
    for s in range(HALVES):
        weigh(0, s)
    steps(1, 1, 3, 2, -8)
    steps(2, 1, 5, 4, 3, -8, -1)
    steps(3, 1, 7, 6, -8, 5, -1, 4, -2)
    for s in range(HALVES):
        finish(1, s)
    for s in range(HALVES):
        weigh(1, s)
    for r in range(ROUNDS):
        for s in range(HALVES):
            merge(r, s)
    for r in range(ROUNDS):
        for s in range(HALVES):
            for dx in (1, 2, 3):
                out_copy(r, s, dx, True).wait_recv()
        out_ref[:, :, :, STARTS[r]:STARTS[r] + WIDTHS[r]] = merged[r][...]

    for dy, dc in ((1, 0), (3, 0), (2, 0), (0, 1)):
        row_copy(dy, dc, False).wait_send()
    for dy in (1, 3, 2):
        row_pass(dy, False).wait_send()

    @pl.loop(0, 4)
    def _(k):
        for r in range(ROUNDS):
            for dy, dc in ((1, 0), (3, 0), (1, 1), (3, 1), (0, 1)):
                col_copy(r, k, dy, dc).wait_send()
            for core in (0, 1):
                col_pass(r, k, core).wait_send()

    for dx in (1, 2, 3):
        w_copy(dx, False).wait_send()
        for r in range(ROUNDS):
            for s in range(HALVES):
                part_copy(r, s, dx, False).wait_send()
                out_copy(r, s, dx, False).wait_send()
    for r in range(ROUNDS):
        for s in range(HALVES):
            for copy in far_copies(r, s):
                copy.wait_send()

    @pl.loop(0, 8)
    def _(away):
        @pl.when(away != place)
        def _():
            for r in range(ROUNDS):
                coded_sent(jnp.where(away > place, main, 1 - main), r, flip(away))


def shards(inputs, cotangent, token_ids, weights):
    seq, feature = inputs.shape[2:]
    query = cotangent.shape[3]
    height, width = weights.shape[2:]
    band = height // HALVES // 4
    blocks = weights[0, 0].reshape(HALVES, 4, band, width)
    vmem = pl.BlockSpec(memory_space=pltpu.VMEM)
    dma = pltpu.SemaphoreType.DMA
    merged = pl.pallas_call(
        kernel,
        out_shape=jax.ShapeDtypeStruct((HALVES, 4, band, width), jnp.float32),
        in_specs=[pl.BlockSpec(memory_space=pl.ANY)] * 3 + [vmem],
        out_specs=vmem,
        scratch_shapes=[
            pltpu.VMEM((seq, feature), jnp.bfloat16),
            pltpu.VMEM((feature, seq), jnp.bfloat16),
            pltpu.VMEM((seq, query), jnp.bfloat16),
            pltpu.VMEM((HALVES, 4, band, width), jnp.float32),
            pltpu.VMEM((8, 2 * height, seq), jnp.bfloat16),
            [pltpu.VMEM((8, 4, seq, part), jnp.bfloat16) for part in WIDTHS],
            [pltpu.VMEM((8, height, part), jnp.float32) for part in WIDTHS],
            [pltpu.VMEM((2, 8, height, part), jnp.bfloat16) for part in WIDTHS],
            [pltpu.VMEM((HALVES, 4, band, part), jnp.float32) for part in WIDTHS],
            [pltpu.VMEM((HALVES, 4, band, part), jnp.float32) for part in WIDTHS],
            pltpu.VMEM((4, HALVES, band, width), jnp.float32),
            [pltpu.VMEM((HALVES, band, part), jnp.float32) for part in WIDTHS],
            [pltpu.VMEM((HALVES, band, part), jnp.bfloat16) for part in WIDTHS],
            [pltpu.VMEM((HALVES, band, part), jnp.float32) for part in WIDTHS],
            [pltpu.VMEM((HALVES, band, part), jnp.bfloat16) for part in WIDTHS],
            [pltpu.VMEM((HALVES, 4, band, part), jnp.float32) for part in WIDTHS],
            dma((3,)),
            dma((8,)), dma((8,)), dma((ROUNDS, 4, 8)), dma((ROUNDS, 4, 8)),
            dma((2, ROUNDS, 8)), dma((2, ROUNDS, 8, SUBS)),
            dma((4,)), dma((4,)), dma((ROUNDS, HALVES, 4)), dma((ROUNDS, HALVES, 4)),
            dma((2, ROUNDS, HALVES)), dma((2, ROUNDS, HALVES)), dma((ROUNDS, HALVES, 4)), dma((ROUNDS, HALVES, 4)),
        ],
        compiler_params=pltpu.CompilerParams(collective_id=0, has_side_effects=True),
    )(inputs[0, 0], cotangent[0, 0], blocks, token_ids[0])
    return merged.reshape(1, height, width)


def solution(mesh):
    in_specs = (
        P("mp", "tok", None, None),
        P("mp", "tok", None, None),
        P("mp", "tok", None),
        P("mp", "tok", None, None),
    )
    out_specs = P("tok", None, None)
    return jax.shard_map(shards, mesh=mesh, in_specs=in_specs, out_specs=out_specs, check_vma=False)
```
